256 devices in a mesh: dp: 16 (over y, x_hi, core), space: 16 (over x_lo, z).
Axes of the slice: x: 4 (x_hi: 2, x_lo: 2; x = x_hi * 2 + x_lo), y: 4, z: 8, core: 2. Of those that a mesh axis runs over, the one named last changes fastest.
Arguments:
- act_in: bfloat16 [16, 32, 64, 2048], P('dp', 'space'), may hold values from -6 to 6
- weight_one: bfloat16 [3, 3, 3, 32, 64], replicated, may hold values from -0.21875 to 0.21875
- bias_one: float32 [64], replicated, may hold values from -3 to 3
- weight_two: bfloat16 [3, 3, 3, 64, 128], replicated, may hold values from -0.15625 to 0.15625
- bias_two: float32 [128], replicated, may hold values from -3 to 3
- cotangent: bfloat16 [16, 16, 32, 4096], P('dp', 'space'), may hold values from -24 to 24
Outputs:
- grad_input: bfloat16 [16, 32, 64, 2048], P('dp', 'space')
- grad_w_one: float32 [3, 3, 3, 32, 64], replicated
- grad_b_one: float32 [64], replicated
- grad_w_two: float32 [3, 3, 3, 64, 128], replicated
- grad_b_two: float32 [128], replicated
The draws below stay inside these ranges and needn't reach their ends.
All inputs are finite; a program needn't handle non-finite values.
Results may differ from the reference program's by a relative error of at most 0.01.
Values may be sent and summed in bfloat16 or wider, within the bound.
A program may use at most 128 MiB of HBM per device.

```python
import math
import jax
import jax.numpy as jnp
from jax import lax

C0 = 32
C1 = 64
C2 = 128
SIDE = 64
BATCH = 16
DEPTH = 32
DEPTH2 = 16
HALF = 32


def levels(rng, shape, shards, smallest, high):
    gain = 1.0
    for dim, blocks in shards:
        draws = jax.random.uniform(jax.random.fold_in(jax.random.fold_in(rng, 6), dim), (blocks,), jnp.float32, smallest / len(shards), high / len(shards))
        gain = gain * jnp.repeat(jnp.exp(draws), shape[dim] // blocks).reshape((-1,) + (1,) * (len(shape) - 1 - dim))
    return gain


def centred(stream_key, dims, deviation, reach, cuts=(), kind=jnp.bfloat16):
    gain = levels(stream_key, dims, cuts, -0.22, 0.18) if cuts else 1.0
    drawn = jax.random.normal(stream_key, dims, jnp.float32) * deviation * gain
    return jnp.minimum(jnp.maximum(drawn, -reach), reach).astype(kind)


def setup_inputs(seed: int = 0) -> dict:
    splits = jax.random.split(jax.random.key(seed), 7)
    return {
        "act_in": centred(splits[0], (BATCH, DEPTH, SIDE, SIDE * C0), 1.0, 6.0, ((0, 16), (1, 16))),
        "weight_one": centred(splits[1], (3, 3, 3, C0, C1), (27 * C0) ** -0.5, 0.21875),
        "bias_one": centred(splits[2], (C1,), 0.5, 3.0, (), jnp.float32),
        "weight_two": centred(splits[3], (3, 3, 3, C1, C2), (27 * C1) ** -0.5, 0.15625),
        "bias_two": centred(splits[4], (C2,), 0.5, 3.0, (), jnp.float32),
        "cotangent": centred(splits[5], (BATCH, DEPTH2, HALF, HALF * C2), 4.0, 24.0, ((0, 16), (1, 16))),
    }


def forward_conv(padded, kernel):
    return lax.conv_general_dilated(padded, kernel, (1, 1, 1), ((0, 0), (1, 1), (1, 1)), dimension_numbers=('NDHWC', 'DHWIO', 'NDHWC'), preferred_element_type=jnp.float32)

def weight_grad(padded, delta):
    return lax.conv_general_dilated(padded, delta, (1, 1, 1), ((0, 0), (1, 1), (1, 1)), dimension_numbers=('CDHWN', 'IDHWO', 'DHWNC'), preferred_element_type=jnp.float32)

def input_grad(delta, kernel, depth_pad):
    return lax.conv_general_dilated(delta, kernel[::-1, ::-1, ::-1], (1, 1, 1), (depth_pad, (1, 1), (1, 1)), dimension_numbers=('NDHWC', 'DHWOI', 'NDHWC'), preferred_element_type=jnp.float32)

def silu_slope(value):
    sig = jax.nn.sigmoid(value)
    return sig * (1.0 + value * (1.0 - sig))

def reference(act_in, weight_one, bias_one, weight_two, bias_two, cotangent):

    def single(pair):
        sample, cot = pair
        x_five = sample.reshape(1, DEPTH, SIDE, SIDE, C0)
        x_pad = jnp.pad(x_five, ((0, 0), (1, 1), (0, 0), (0, 0), (0, 0)))
        pre_one = forward_conv(x_pad, weight_one) + bias_one
        act_one = pre_one * jax.nn.sigmoid(pre_one)
        pooled = act_one.reshape(1, DEPTH2, 2, HALF, 2, HALF, 2, C1).mean(axis=(2, 4, 6)).astype(jnp.bfloat16)
        pool_pad = jnp.pad(pooled, ((0, 0), (1, 1), (0, 0), (0, 0), (0, 0)))
        pre_two = forward_conv(pool_pad, weight_two) + bias_two
        cot_five = cot.reshape(1, DEPTH2, HALF, HALF, C2).astype(jnp.float32)
        delta_two = (cot_five * silu_slope(pre_two)).astype(jnp.bfloat16)
        gw_two = weight_grad(pool_pad, delta_two)
        gb_two = lax.optimization_barrier(jnp.sum(delta_two, axis=(0, 1, 2, 3), dtype=jnp.float32))
        grad_pooled = input_grad(delta_two, weight_two, (1, 1))
        spread = jnp.broadcast_to(grad_pooled[:, :, None, :, None, :, None, :], (1, DEPTH2, 2, HALF, 2, HALF, 2, C1)).reshape(1, DEPTH, SIDE, SIDE, C1)
        delta_one = (spread / 8.0 * silu_slope(pre_one)).astype(jnp.bfloat16)
        gw_one = weight_grad(x_pad, delta_one)
        gb_one = lax.optimization_barrier(jnp.sum(delta_one, axis=(0, 1, 2, 3), dtype=jnp.float32))
        grad_x = input_grad(delta_one, weight_one, (1, 1)).astype(jnp.bfloat16).reshape(DEPTH, SIDE, SIDE * C0)
        return (grad_x, gw_one, gb_one, gw_two, gb_two)
    grad_x, gw_one, gb_one, gw_two, gb_two = lax.map(single, (act_in, cotangent))
    scale_one = 16.0 / math.sqrt(BATCH * DEPTH * SIDE * SIDE)
    scale_two = 1.0 / math.sqrt(BATCH * DEPTH2 * HALF * HALF)
    return (grad_x, lax.optimization_barrier(jnp.sum(gw_one, axis=0)) * scale_one, lax.optimization_barrier(jnp.sum(gb_one, axis=0)) * scale_one, lax.optimization_barrier(jnp.sum(gw_two, axis=0)) * scale_two, lax.optimization_barrier(jnp.sum(gb_two, axis=0)) * scale_two)
```

```python
import functools
import math

import jax
import jax.numpy as jnp
from jax import lax
from jax.experimental import pallas as pl
from jax.experimental.pallas import tpu as pltpu
from jax.sharding import PartitionSpec as P

F32 = jnp.float32
BF16 = jnp.bfloat16
LINK = jnp.float32
MESH = pl.DeviceIdType.MESH

E0, O0, EP, OM = 0, 1, 2, 3
FWD = ((OM, E0, O0), (E0, O0, EP))
BWD = ((O0, E0, OM), (EP, O0, E0))

NT = (((1,), (1,)), ((), ()))
TN = (((0,), (0,)), ((), ()))


def dot(a, b):
    return jnp.dot(a, b, preferred_element_type=F32)


def slope_of(value, sig):
    return sig * (1.0 + value * (1.0 - sig))


def sigmoid(value):
    return 0.5 * jnp.tanh(0.5 * value) + 0.5


def kernel(
    scale_one, scale_two,
    x_ref, w1_ref, b1_ref, w2_ref, b2_ref, cot_ref,
    gx_ref, gw1_ref, gb1_ref, gw2_ref, gb2_ref,
    t1, t2, xf, xv, halo_x, slope, pf, pool, halo_p, ps, d2, gsend, grecv, gown, gp,
    d1, d1t, xsend, xrecv, xown, outf,
    acc, r0, half, r1, r2, final,
    s_send, s_recv, a_send, a_recv, z_send, z_recv, g_send, g_recv, c_send, c_recv,
):
    dp = lax.axis_index("dp")
    space = lax.axis_index("space")
    nxt = lax.rem(space + 1, 16)
    prv = lax.rem(space + 15, 16)
    core = lax.rem(dp, 2)
    x_pos = lax.rem(dp // 2, 2) * 2 + space // 8
    chip = (dp // 4) * 4 + x_pos
    z = lax.rem(space, 8)
    partner = (dp + 1 - 2 * core, space)

    def chip_at(r):
        q = lax.rem(chip + r, 16)
        qx = lax.rem(q, 4)
        return (q // 4) * 4 + (qx // 2) * 2 + core, lax.rem(qx, 2) * 8 + z, q

    def z_at(r):
        return dp, (space // 8) * 8 + lax.rem(z + r, 8)

    barrier = pltpu.get_barrier_semaphore()

    def greet(device):
        pl.semaphore_signal(barrier, inc=1, device_id=device, device_id_type=MESH)

    greet((dp, nxt))
    greet((dp, prv))
    greet(partner)
    for r in range(1, 16):
        greet(chip_at(r)[:2])
    for r in range(1, 8):
        greet(z_at(r))

    for k in range(3):
        for j in range(3):
            w = w1_ref[k, j].reshape(96, 64).astype(F32)
            for t in range(2):
                cols = []
                for v in (t, t + 2):
                    parts = [w]
                    if v:
                        parts = [jnp.zeros((32 * v, 64), F32)] + parts
                    parts = parts + [jnp.zeros((160 - 32 * v, 64), F32)]
                    cols.append(jnp.concatenate(parts, axis=0))
                t1[pl.ds((k * 3 + j) * 256, 256), pl.ds(t * 128, 128)] = jnp.concatenate(cols, axis=1).astype(BF16)
            w = w2_ref[k, j].reshape(192, 128)
            gap = jnp.zeros((64, 128), BF16)
            t2[pl.ds((k * 3 + j) * 256, 256), pl.ds(0, 128)] = jnp.concatenate([w, gap], axis=0)
            t2[pl.ds((k * 3 + j) * 256, 256), pl.ds(128, 128)] = jnp.concatenate([gap, w], axis=0)

    pl.semaphore_wait(barrier, 25)

    def exchange(down, up, from_next, from_prev, stage):
        one = pltpu.make_async_remote_copy(
            src_ref=down, dst_ref=from_next, send_sem=s_send.at[stage, 0], recv_sem=s_recv.at[stage, 0],
            device_id=(dp, prv), device_id_type=MESH)
        two = pltpu.make_async_remote_copy(
            src_ref=up, dst_ref=from_prev, send_sem=s_send.at[stage, 1], recv_sem=s_recv.at[stage, 1],
            device_id=(dp, nxt), device_id_type=MESH)
        one.start()
        two.start()
        return one, two

    def finish(pair):
        pair[0].wait()
        pair[1].wait()

    not_last = space < 15
    not_first = space > 0

    pair = exchange(x_ref.at[0, 0], x_ref.at[0, 1], halo_x.at[1], halo_x.at[0], 0)

    xf[:, 0:8, :] = jnp.zeros((17, 8, 128), F32)
    xf[:, 72:80, :] = jnp.zeros((17, 8, 128), F32)
    lane = lax.broadcasted_iota(jnp.int32, (16, 128), 1)

    def prepare(src, plane, keep):
        def rows(i, carry):
            v = src[pl.ds(pl.multiple_of(i * 16, 16), 16), :].astype(F32)
            if keep is not None:
                v = jnp.where(keep, v, 0.0)
            v = pltpu.roll(v, 32, 1)
            at = pl.ds(pl.multiple_of(i * 16 + 8, 8), 16)
            xf[0, at, :] = jnp.where(lane < 32, 0.0, v[:, 0:128])
            for t in range(1, 16):
                xf[t, at, :] = v[:, t * 128:t * 128 + 128]
            xf[16, at, :] = jnp.where(lane < 32, v[:, 0:128], 0.0)
            return carry
        lax.fori_loop(0, 4, rows, 0)

        def tiles(i, carry):
            at = pl.ds(pl.multiple_of(i * 128, 128), 128)
            xv[plane, E0, :, at] = xf[i, pl.ds(8, 32, stride=2), :].astype(BF16)
            xv[plane, O0, :, at] = xf[i, pl.ds(9, 32, stride=2), :].astype(BF16)
            xv[plane, EP, :, at] = xf[i, pl.ds(10, 32, stride=2), :].astype(BF16)
            xv[plane, OM, :, at] = xf[i, pl.ds(7, 32, stride=2), :].astype(BF16)
            return carry
        lax.fori_loop(0, 17, tiles, 0)

    prepare(x_ref.at[0, 0], 1, None)
    prepare(x_ref.at[0, 1], 2, None)
    finish(pair)
    prepare(halo_x.at[0], 0, not_first)
    prepare(halo_x.at[1], 3, not_last)

    bias = jnp.concatenate([b1_ref[...], b1_ref[...]], axis=1)
    bias = jnp.concatenate([bias, bias], axis=1)

    def forward_one(g, carry):
        sums = [None] * 4
        for d in range(2):
            for p in range(2):
                lhs = jnp.concatenate([
                    jnp.concatenate([
                        xv[d + k, FWD[p][j], :, pl.ds(pl.multiple_of((g * 4 + b) * 128, 128), 256)]
                        for b in range(4)], axis=0)
                    for k in range(3) for j in range(3)], axis=1)
                pre = dot(lhs, t1[...]) + bias
                sig = sigmoid(pre)
                act = pre * sig
                slope[d * 2 + p, pl.ds(pl.multiple_of(g * 128, 128), 128), :] = slope_of(pre, sig) * 0.125
                for b in range(4):
                    part = act[b * 32:b * 32 + 32, 0:128] + act[b * 32:b * 32 + 32, 128:256]
                    sums[b] = part if sums[b] is None else sums[b] + part
        for b in range(4):
            pool[:, pl.ds(pl.multiple_of((g * 4 + b) * 128, 128), 128)] = (sums[b] * 0.125).astype(BF16)
        return carry
    lax.fori_loop(0, 4, forward_one, 0)

    pair = exchange(pool, pool, halo_p.at[1], halo_p.at[0], 1)

    pf[0:8, :] = jnp.zeros((8, 2176), F32)
    pf[40:48, :] = jnp.zeros((8, 2176), F32)
    lane_p = lax.broadcasted_iota(jnp.int32, (32, 2048), 1)
    lane_q = lax.broadcasted_iota(jnp.int32, (32, 128), 1)

    def prepare_pool(src, plane, keep):
        v = src[...].astype(F32)
        if keep is not None:
            v = jnp.where(keep, v, 0.0)
        v = pltpu.roll(v, 64, 1)
        pf[8:40, 0:2048] = jnp.where(lane_p < 64, 0.0, v)
        pf[8:40, 2048:2176] = jnp.where(lane_q < 64, v[:, 0:128], 0.0)
        for j in range(3):
            ps[plane, j] = pf[7 + j:39 + j, :].astype(BF16)

    prepare_pool(pool, 1, None)
    finish(pair)
    prepare_pool(halo_p.at[0], 0, not_first)
    prepare_pool(halo_p.at[1], 2, not_last)

    row = lax.broadcasted_iota(jnp.int32, (32, 256), 0)
    bias_two = jnp.concatenate([b2_ref[...], b2_ref[...]], axis=1)

    def shift_up(v):
        return jnp.where(row < 31, pltpu.roll(v, 31, 0), 0.0)

    def shift_down(v):
        return jnp.where(row > 0, pltpu.roll(v, 1, 0), 0.0)

    def forward_two(g, total):
        lhs = jnp.concatenate([
            jnp.concatenate([
                ps[k, j, :, pl.ds(pl.multiple_of((g * 4 + b) * 128, 128), 256)] for b in range(4)], axis=0)
            for k in range(3) for j in range(3)], axis=1)
        pre = dot(lhs, t2[...]) + bias_two
        slp = slope_of(pre, sigmoid(pre))
        for b in range(4):
            at = pl.ds(pl.multiple_of((g * 4 + b) * 256, 256), 256)
            rows = pl.ds(pl.multiple_of((g * 4 + b) * 32, 32), 32)
            delta = (cot_ref[0, 0, :, at].astype(F32) * slp[b * 32:b * 32 + 32]).astype(BF16)
            wide = delta.astype(F32)
            d2[1, rows, :] = delta
            d2[0, rows, :] = shift_up(wide).astype(BF16)
            d2[2, rows, :] = shift_down(wide).astype(BF16)
            total = total + wide
        return total
    total_two = lax.fori_loop(0, 4, forward_two, jnp.zeros((32, 256), F32))

    def window_tiles(win, put):
        for t in range(17):
            piece = None
            if t < 16:
                piece = win[t * 32:t * 32 + 32, 0:128]
            if t > 0:
                other = win[t * 32 - 32:t * 32, 128:256]
                piece = other if piece is None else piece + other
            put(t, piece)

    lhs_two = jnp.concatenate([d2[0], d2[1], d2[2]], axis=1)
    for k in (0, 2, 1):
        rhs = jnp.concatenate([t2[pl.ds((k * 3 + j) * 256, 256), :] for j in range(3)], axis=1)
        win = lax.dot_general(lhs_two, rhs, NT, preferred_element_type=F32)
        if k == 1:
            def put(t, piece):
                gown[:, t * 128:t * 128 + 128] = piece
        else:
            def put(t, piece, k=k):
                gsend[k // 2, :, t * 128:t * 128 + 128] = piece.astype(BF16)
        window_tiles(win, put)
    pair = exchange(gsend.at[0], gsend.at[1], grecv.at[1], grecv.at[0], 2)

    for k in range(3):
        for j in range(3):
            lhs = jnp.concatenate([ps[k, j, :, b * 128:b * 128 + 256] for b in range(16)], axis=0)
            g = lax.dot_general(lhs, d2[1], TN, preferred_element_type=F32)
            acc_rows = g[0:192, 0:128] + g[64:256, 128:256]
            for part in range(8):
                tap = k * 3 + j
                first = tap * 192 + part * 24
                acc[first // 72, pl.ds(first % 72, 24), :] = acc_rows[part * 24:part * 24 + 24]

    finish(pair)
    v = gown[...]
    v = v + jnp.where(not_first, grecv[0].astype(F32), 0.0) + jnp.where(not_last, grecv[1].astype(F32), 0.0)
    v = pltpu.roll(v, 2176 - 64, 1)
    gp[...] = v[:, 0:2048]

    def delta_one(b, total):
        g = gp[:, pl.ds(pl.multiple_of(b * 128, 128), 128)]
        g = jnp.concatenate([g, g], axis=1)
        rows = pl.ds(pl.multiple_of(b * 32, 32), 32)
        for d in range(2):
            for p in range(2):
                delta = (g * slope[d * 2 + p, rows, :]).astype(BF16)
                wide = delta.astype(F32)
                d1[d, E0 if p == 0 else O0, rows, :] = delta
                if p == 0:
                    d1[d, EP, rows, :] = shift_up(wide).astype(BF16)
                else:
                    d1[d, OM, rows, :] = shift_down(wide).astype(BF16)
                total = total + wide
        return total
    total_one = lax.fori_loop(0, 16, delta_one, jnp.zeros((32, 256), F32))

    def window_one(terms, q):
        lhs = jnp.concatenate([d1[d, BWD[q][j]] for d, k in terms for j in range(3)], axis=1)
        rhs = jnp.concatenate([t1[pl.ds((k * 3 + j) * 256, 256), :] for d, k in terms for j in range(3)], axis=1)
        return lax.dot_general(lhs, rhs, NT, preferred_element_type=F32)

    for side, terms in ((0, ((0, 0),)), (1, ((1, 2),))):
        for q in range(2):
            def put(t, piece, side=side, q=q):
                xsend[side, q, :, t * 128:t * 128 + 128] = piece.astype(BF16)
            window_tiles(window_one(terms, q), put)
    pair = exchange(xsend.at[0], xsend.at[1], xrecv.at[1], xrecv.at[0], 3)

    for d in range(2):
        for p in range(2):
            for c in range(4):
                v = d1[d, p, pl.ds(c * 128, 128), :]
                d1t[:, pl.ds((d * 2 + p) * 512 + c * 128, 128)] = jnp.transpose(v)

    total = jnp.sum(total_one, axis=0, keepdims=True)
    total = total[:, 0:128] + total[:, 128:256]
    total = total + pltpu.roll(total, 64, 1)
    low = lax.broadcasted_iota(jnp.int32, (64, 128), 1)
    total_col = jnp.sum(
        jnp.where(low == lax.broadcasted_iota(jnp.int32, (64, 128), 0), total, 0.0), axis=1, keepdims=True)
    two = jnp.sum(total_two, axis=0, keepdims=True)
    two = jnp.broadcast_to(two[:, 0:128] + two[:, 128:256], (8, 128))
    for k in range(3):
        for j in range(3):
            tap = k * 3 + j
            rhs = jnp.concatenate([
                xv[d + k, FWD[p][j], :, b * 128:b * 128 + 256]
                for d in range(2) for p in range(2) for b in range(16)], axis=0)
            g = dot(d1t[...], rhs)
            s = g[0:64, 0:128] + pltpu.roll(g[128:192, 0:256], 256 - 32, 1)[:, 0:128]
            s = s + pltpu.roll(g[64:128, 0:256], 256 - 64, 1)[:, 0:128]
            s = s + pltpu.roll(g[192:256, 0:256], 256 - 96, 1)[:, 0:128]
            if tap == 0:
                s = jnp.where(low < 96, s, total_col)
            if tap == 1:
                extra = jnp.zeros((8, 128), F32)
                sub = lax.broadcasted_iota(jnp.int32, (8, 128), 0)
                for quarter in range(4):
                    moved = pltpu.roll(two, (96 - 32 * quarter) % 128, 1) if quarter != 3 else two
                    extra = jnp.where(sub == quarter, moved, extra)
                s = jnp.where(low < 96, s, jnp.concatenate([extra] * 8, axis=0))
            for part in range(8):
                first = 1728 + tap * 64 + part * 8
                acc[first // 72, pl.ds(first % 72, 8), :] = s[part * 8:part * 8 + 8]

    swap = pltpu.make_async_remote_copy(
        src_ref=acc.at[pl.ds((1 - core) * 16, 16)], dst_ref=r0, send_sem=c_send.at[0], recv_sem=c_recv.at[0],
        device_id=partner, device_id_type=MESH)
    swap.start()

    def own_planes(e, terms):
        for q in range(2):
            def put(t, piece, q=q):
                xown[e, q, :, t * 128:t * 128 + 128] = piece
            window_tiles(window_one(terms, q), put)
    own_planes(0, ((0, 1), (1, 0)))
    swap.wait()

    def add_half(i, carry):
        half[i] = (acc[core * 16 + i] + r0[i]).astype(LINK)
        return carry
    lax.fori_loop(0, 16, add_half, 0)
    sends = []
    for r in range(1, 16):
        a, b, q = chip_at(r)
        cp = pltpu.make_async_remote_copy(
            src_ref=half.at[q], dst_ref=r1.at[r - 1], send_sem=a_send.at[r - 1], recv_sem=a_recv.at[r - 1],
            device_id=(a, b), device_id_type=MESH)
        cp.start()
        sends.append(cp)
    own_planes(1, ((0, 2), (1, 1)))
    piece = half[chip].astype(F32)
    for r in range(1, 16):
        sends[r - 1].wait()
        piece = piece + r1[r - 1].astype(F32)
    r2[z] = piece.astype(LINK)
    sends = []
    for r in range(1, 8):
        cp = pltpu.make_async_remote_copy(
            src_ref=r2.at[z], dst_ref=r2.at[z], send_sem=z_send.at[r - 1], recv_sem=z_recv.at[r - 1],
            device_id=z_at(r), device_id_type=MESH)
        cp.start()
        sends.append(cp)

    finish(pair)
    for e in range(2):
        for q in range(2):
            halo = xrecv[e, q].astype(F32)
            v = xown[e, q] + jnp.where(not_first if e == 0 else not_last, halo, 0.0)
            v = pltpu.roll(v, 2176 - 32, 1)[:, 0:2048]
            for t in range(16):
                outf[t, pl.ds(q, 32, stride=2), :] = v[:, t * 128:t * 128 + 128]
        for t in range(16):
            gx_ref[0, e, :, t * 128:t * 128 + 128] = outf[t].astype(BF16)

    for cp in sends:
        cp.wait()
    piece = r2[0].astype(F32)
    for i in range(1, 8):
        piece = piece + r2[i].astype(F32)
    mine = core * 16 + chip
    final[mine] = piece.astype(LINK)
    sends = []
    for r in range(1, 16):
        a, b, q = chip_at(r)
        cp = pltpu.make_async_remote_copy(
            src_ref=final.at[mine], dst_ref=final.at[mine], send_sem=g_send.at[r - 1], recv_sem=g_recv.at[r - 1],
            device_id=(a, b), device_id_type=MESH)
        cp.start()
        sends.append(cp)
    for cp in sends:
        cp.wait()
    swap = pltpu.make_async_remote_copy(
        src_ref=final.at[pl.ds(core * 16, 16)], dst_ref=final.at[pl.ds(core * 16, 16)],
        send_sem=c_send.at[1], recv_sem=c_recv.at[1], device_id=partner, device_id_type=MESH)
    swap.start()
    swap.wait()

    for tap in range(9):
        for i in range(3):
            rows = []
            for part in range(8):
                first = tap * 192 + i * 64 + part * 8
                rows.append(final[first // 72, pl.ds(first % 72, 8), :].astype(F32))
            gw2_ref[tap // 3, tap % 3, i] = jnp.concatenate(rows, axis=0) * scale_two
        rows = []
        for part in range(8):
            first = 1728 + tap * 64 + part * 8
            rows.append(final[first // 72, pl.ds(first % 72, 8), :].astype(F32))
        s = jnp.concatenate(rows, axis=0)
        turned = jnp.transpose(s)
        for i in range(3):
            gw1_ref[tap // 3, tap % 3, i] = turned[i * 32:i * 32 + 32] * scale_one
        if tap == 0:
            gb1_ref[...] = turned[96:97] * scale_one
        if tap == 1:
            lane_one = lax.broadcasted_iota(jnp.int32, (1, 128), 1)
            out = jnp.zeros((1, 128), F32)
            for quarter in range(4):
                moved = s[quarter:quarter + 1]
                if quarter != 3:
                    moved = pltpu.roll(moved, 32 + 32 * quarter, 1)
                out = jnp.where(lane_one // 32 == quarter, moved, out)
            gb2_ref[...] = out * scale_two


def local(act_in, weight_one, bias_one, weight_two, bias_two, cotangent):
    scale_one = 16.0 / math.sqrt(16 * 32 * 64 * 64)
    scale_two = 1.0 / math.sqrt(16 * 16 * 32 * 32)
    vmem = pl.BlockSpec(memory_space=pltpu.VMEM)
    scratch = [
        pltpu.VMEM((2304, 256), BF16),
        pltpu.VMEM((2304, 256), BF16),
        pltpu.VMEM((17, 80, 128), F32),
        pltpu.VMEM((4, 4, 32, 2176), BF16),
        pltpu.VMEM((2, 64, 2048), BF16),
        pltpu.VMEM((4, 512, 256), F32),
        pltpu.VMEM((48, 2176), F32),
        pltpu.VMEM((32, 2048), BF16),
        pltpu.VMEM((2, 32, 2048), BF16),
        pltpu.VMEM((3, 3, 32, 2176), BF16),
        pltpu.VMEM((3, 512, 256), BF16),
        pltpu.VMEM((2, 32, 2176), BF16),
        pltpu.VMEM((2, 32, 2176), BF16),
        pltpu.VMEM((32, 2176), F32),
        pltpu.VMEM((32, 2048), F32),
        pltpu.VMEM((2, 4, 512, 256), BF16),
        pltpu.VMEM((256, 2048), BF16),
        pltpu.VMEM((2, 2, 32, 2176), BF16),
        pltpu.VMEM((2, 2, 32, 2176), BF16),
        pltpu.VMEM((2, 2, 32, 2176), F32),
        pltpu.VMEM((16, 64, 128), F32),
        pltpu.VMEM((32, 72, 128), F32),
        pltpu.VMEM((16, 72, 128), F32),
        pltpu.VMEM((16, 72, 128), LINK),
        pltpu.VMEM((15, 72, 128), LINK),
        pltpu.VMEM((8, 72, 128), LINK),
        pltpu.VMEM((32, 72, 128), LINK),
        pltpu.SemaphoreType.DMA((4, 2)),
        pltpu.SemaphoreType.DMA((4, 2)),
        pltpu.SemaphoreType.DMA((15,)),
        pltpu.SemaphoreType.DMA((15,)),
        pltpu.SemaphoreType.DMA((7,)),
        pltpu.SemaphoreType.DMA((7,)),
        pltpu.SemaphoreType.DMA((15,)),
        pltpu.SemaphoreType.DMA((15,)),
        pltpu.SemaphoreType.DMA((2,)),
        pltpu.SemaphoreType.DMA((2,)),
    ]
    gx, gw1, gb1, gw2, gb2 = pl.pallas_call(
        functools.partial(kernel, scale_one, scale_two),
        out_shape=(
            jax.ShapeDtypeStruct((1, 2, 64, 2048), BF16),
            jax.ShapeDtypeStruct((3, 3, 3, 32, 64), F32),
            jax.ShapeDtypeStruct((1, 64), F32),
            jax.ShapeDtypeStruct((3, 3, 3, 64, 128), F32),
            jax.ShapeDtypeStruct((1, 128), F32),
        ),
        in_specs=[vmem] * 6,
        out_specs=(vmem,) * 5,
        scratch_shapes=scratch,
        compiler_params=pltpu.CompilerParams(
            collective_id=0, has_side_effects=True, vmem_limit_bytes=60 * 1024 * 1024),
    )(act_in, weight_one, bias_one.reshape(1, 64), weight_two, bias_two.reshape(1, 128), cotangent)
    return gx, gw1, gb1.reshape(64), gw2, gb2.reshape(128)


def solution(mesh):
    placed = (P("dp", "space", None, None), P(), P(), P(), P(), P("dp", "space", None, None))
    return jax.shard_map(
        local,
        mesh=mesh,
        in_specs=placed,
        out_specs=(P("dp", "space", None, None), P(), P(), P(), P()),
        check_vma=False,
    )
```

```python
import functools
import math

import jax
import jax.numpy as jnp
from jax import lax
from jax.experimental import pallas as pl
from jax.experimental.pallas import tpu as pltpu
from jax.sharding import PartitionSpec as P

F32 = jnp.float32
BF16 = jnp.bfloat16
LINK1 = jnp.bfloat16
LINK2 = jnp.bfloat16
MESH = pl.DeviceIdType.MESH

E0, O0, EP, OM = 0, 1, 2, 3
FWD = ((OM, E0, O0), (E0, O0, EP))
BWD = ((O0, E0, OM), (EP, O0, E0))

NT = (((1,), (1,)), ((), ()))
TN = (((0,), (0,)), ((), ()))

X_CUT = (0, 9, 16)
ROWS2 = 56
ROWS1 = 16


def dot(a, b):
    return jnp.dot(a, b, preferred_element_type=F32)


def slope_of(value, sig):
    return sig * (1.0 + value * (1.0 - sig))


def sigmoid(value):
    return 0.5 * jnp.tanh(0.5 * value) + 0.5


def kernel(
    x_hbm, w1_hbm, b1_hbm, w2_hbm, b2_hbm, cot_hbm,
    gx_buf, fin1, fin2,
    x_a, x_b, w1_ref, b1_ref, w2_ref, b2_ref, cot_ref,
    t1, t2, xf, xv, halo_a, halo_b, slope, pf, pool, halo_p, ps, pre_two, d2, gs_a, gs_b, gr_a, gr_b, gown,
    d1, d1t, xsend, xrecv, xown, outf,
    acc1, half1, r11, r21,
    acc2, r02, half2, r12, r22,
    l_sem, s_send, s_recv, a_send, a_recv, z_send, z_recv, g_send, g_recv, c_send, c_recv, b_send, b_recv,
):
    dp = lax.axis_index("dp")
    space = lax.axis_index("space")
    nxt = lax.rem(space + 1, 16)
    prv = lax.rem(space + 15, 16)
    core = lax.rem(dp, 2)
    x_pos = lax.rem(dp // 2, 2) * 2 + space // 8
    chip = (dp // 4) * 4 + x_pos
    z = lax.rem(space, 8)
    partner = (dp + 1 - 2 * core, space)

    def chip_at(r):
        q = lax.rem(chip + r, 16)
        qx = lax.rem(q, 4)
        return (q // 4) * 4 + (qx // 2) * 2 + core, lax.rem(qx, 2) * 8 + z, q

    def other_at(r):
        da, db, q = chip_at(r)
        return da + 1 - 2 * core, db, q

    def z_at(r):
        return dp, (space // 8) * 8 + lax.rem(z + r, 8)

    barrier = pltpu.get_barrier_semaphore()

    def greet(device):
        pl.semaphore_signal(barrier, inc=1, device_id=device, device_id_type=MESH)

    loads = []
    for i, (src, dst) in enumerate((
        (x_hbm.at[0, :, :, pl.ds(0, 1152)], x_a), (x_hbm.at[0, :, :, pl.ds(1152, 896)], x_b),
        (w1_hbm, w1_ref), (w2_hbm, w2_ref), (b1_hbm, b1_ref), (b2_hbm, b2_ref), (cot_hbm, cot_ref),
    )):
        cp = pltpu.make_async_copy(src, dst, l_sem.at[i])
        cp.start()
        loads.append(cp)

    greet((dp, nxt))
    greet((dp, prv))
    for r in range(1, 8):
        greet(z_at(r))
    for r in range(1, 16):
        greet(chip_at(r)[:2])
    for r in range(16):
        greet(other_at(r)[:2])

    not_last = space < 15
    not_first = space > 0

    def exchange(down, up, from_next, from_prev, stage):
        one = pltpu.make_async_remote_copy(
            src_ref=down, dst_ref=from_next, send_sem=s_send.at[stage, 0], recv_sem=s_recv.at[stage, 0],
            device_id=(dp, prv), device_id_type=MESH)
        two = pltpu.make_async_remote_copy(
            src_ref=up, dst_ref=from_prev, send_sem=s_send.at[stage, 1], recv_sem=s_recv.at[stage, 1],
            device_id=(dp, nxt), device_id_type=MESH)

        @pl.when(not_first)
        def _():
            one.start()

        @pl.when(not_last)
        def _():
            two.start()
        return one, two

    def finish(pair):
        one, two = pair

        @pl.when(not_first)
        def _():
            one.wait_send()
            two.wait_recv()

        @pl.when(not_last)
        def _():
            two.wait_send()
            one.wait_recv()

    loads[0].wait()
    loads[1].wait()
    pl.semaphore_wait(barrier, 40)
    x_pairs = [
        exchange(x_a.at[0], x_a.at[1], halo_a.at[1], halo_a.at[0], 0),
        exchange(x_b.at[0], x_b.at[1], halo_b.at[1], halo_b.at[0], 1),
    ]

    @pl.when(jnp.logical_not(not_first))
    def _():
        halo_a[0] = jnp.zeros(halo_a.shape[1:], BF16)
        halo_b[0] = jnp.zeros(halo_b.shape[1:], BF16)
        halo_p[0] = jnp.zeros(halo_p.shape[1:], BF16)
        gr_a[0] = jnp.zeros(gr_a.shape[1:], BF16)
        gr_b[0] = jnp.zeros(gr_b.shape[1:], BF16)
        xrecv[0] = jnp.zeros(xrecv.shape[1:], BF16)

    @pl.when(jnp.logical_not(not_last))
    def _():
        halo_a[1] = jnp.zeros(halo_a.shape[1:], BF16)
        halo_b[1] = jnp.zeros(halo_b.shape[1:], BF16)
        halo_p[1] = jnp.zeros(halo_p.shape[1:], BF16)
        gr_a[1] = jnp.zeros(gr_a.shape[1:], BF16)
        gr_b[1] = jnp.zeros(gr_b.shape[1:], BF16)
        xrecv[1] = jnp.zeros(xrecv.shape[1:], BF16)

    lane = lax.broadcasted_iota(jnp.int32, (64, 128), 1)

    def prepare(src, side, plane, first, last):
        def turned(t):
            if t < 0 or t > 15:
                return jnp.zeros((64, 128), F32)
            c = 0 if t < X_CUT[1] else 1
            v = src[c][side, :, (t - X_CUT[c]) * 128:(t - X_CUT[c]) * 128 + 128].astype(F32)
            return pltpu.roll(v, 32, 1)
        before = turned(first - 1)
        for t in range(first, last):
            here = turned(t)
            xf[t, 8:72, :] = jnp.where(lane < 32, before, here)
            before = here
            at = pl.ds(t * 128, 128)
            xv[plane, E0, :, at] = xf[t, pl.ds(8, 32, stride=2), :].astype(BF16)
            xv[plane, O0, :, at] = xf[t, pl.ds(9, 32, stride=2), :].astype(BF16)
            xv[plane, EP, :, at] = xf[t, pl.ds(10, 32, stride=2), :].astype(BF16)
            xv[plane, OM, :, at] = xf[t, pl.ds(7, 32, stride=2), :].astype(BF16)

    xf[:, 0:8, :] = jnp.zeros((17, 8, 128), F32)
    xf[:, 72:80, :] = jnp.zeros((17, 8, 128), F32)
    pf[0:8, :] = jnp.zeros((8, 2176), F32)
    pf[40:48, :] = jnp.zeros((8, 2176), F32)

    loads[2].wait()
    for k in range(3):
        for j in range(3):
            w = w1_ref[k, j].reshape(96, 64).astype(F32)
            for t in range(2):
                cols = []
                for v in (t, t + 2):
                    parts = [w]
                    if v:
                        parts = [jnp.zeros((32 * v, 64), F32)] + parts
                    parts = parts + [jnp.zeros((160 - 32 * v, 64), F32)]
                    cols.append(jnp.concatenate(parts, axis=0))
                t1[pl.ds((k * 3 + j) * 256, 256), pl.ds(t * 128, 128)] = jnp.concatenate(cols, axis=1).astype(BF16)

    prepare((x_a, x_b), 0, 1, 0, 17)
    prepare((x_a, x_b), 1, 2, 0, 17)

    for i in range(3, 7):
        loads[i].wait()
    for k in range(3):
        for j in range(3):
            w = w2_ref[k, j].reshape(192, 128)
            gap = jnp.zeros((64, 128), BF16)
            t2[pl.ds((k * 3 + j) * 256, 256), pl.ds(0, 128)] = jnp.concatenate([w, gap], axis=0)
            t2[pl.ds((k * 3 + j) * 256, 256), pl.ds(128, 128)] = jnp.concatenate([gap, w], axis=0)

    bias = jnp.concatenate([b1_ref[...], b1_ref[...]], axis=1)
    bias = jnp.concatenate([bias, bias], axis=1)

    def lhs_one(d, ks, first, blocks):
        return jnp.concatenate([
            jnp.concatenate([
                xv[d + k, FWD[p][j], :, pl.ds(pl.multiple_of((first + b) * 128, 128), 256)]
                for p in range(2) for b in range(blocks)], axis=0)
            for k in ks for j in range(3)], axis=1)

    def own_one(g, carry):
        for d in range(2):
            part = dot(lhs_one(d, (1 - d, 2 - d), g * 8, 8), t1[pl.ds((1 - d) * 768, 1536), :])
            for p in range(2):
                slope[d * 2 + p, pl.ds(pl.multiple_of(g * 256, 256), 256), :] = part[p * 256:p * 256 + 256]
        return carry
    lax.fori_loop(0, 2, own_one, 0)

    p_pairs = []
    for g in range(2):
        finish(x_pairs[g])
        prepare((halo_a, halo_b), 0, 0, (0, 9)[g], (9, 17)[g])
        prepare((halo_a, halo_b), 1, 3, (0, 9)[g], (9, 17)[g])
        sums = [None] * 8
        rows = pl.ds(g * 256, 256)
        for d in range(2):
            part = dot(lhs_one(d, (2 * d,), g * 8, 8), t1[pl.ds(2 * d * 768, 768), :])
            for p in range(2):
                pre = part[p * 256:p * 256 + 256] + slope[d * 2 + p, rows, :] + bias
                sig = sigmoid(pre)
                act = pre * sig
                slope[d * 2 + p, rows, :] = slope_of(pre, sig) * 0.125
                for b in range(8):
                    piece = act[b * 32:b * 32 + 32, 0:128] + act[b * 32:b * 32 + 32, 128:256]
                    sums[b] = piece if sums[b] is None else sums[b] + piece
        for b in range(8):
            pool[g, :, b * 128:b * 128 + 128] = (sums[b] * 0.125).astype(BF16)
        p_pairs.append(exchange(pool.at[g], pool.at[g], halo_p.at[1, g], halo_p.at[0, g], 2 + g))

    lane_p = lax.broadcasted_iota(jnp.int32, (32, 128), 1)

    def prepare_pool(src, plane, first, last):
        def turned(t):
            if t < 0 or t > 15:
                return jnp.zeros((32, 128), F32)
            v = src[t // 8, :, t % 8 * 128:t % 8 * 128 + 128].astype(F32)
            return pltpu.roll(v, 64, 1)
        before = turned(first - 1)
        for t in range(first, last):
            here = turned(t)
            at = pl.ds(t * 128, 128)
            pf[8:40, at] = jnp.where(lane_p < 64, before, here)
            before = here
            for j in range(3):
                ps[plane, j, :, at] = pf[7 + j:39 + j, at].astype(BF16)

    def lhs_two(ks, first, blocks):
        return jnp.concatenate([
            jnp.concatenate([ps[k, j, :, pl.ds((first + b) * 128, 256)] for b in range(blocks)], axis=0)
            for k in ks for j in range(3)], axis=1)

    prepare_pool(pool, 1, 0, 17)
    pre_two[...] = dot(lhs_two((1,), 0, 16), t2[pl.ds(768, 768), :])

    row = lax.broadcasted_iota(jnp.int32, (32, 256), 0)
    bias_two = jnp.concatenate([b2_ref[...], b2_ref[...]], axis=1)

    def shift_up(v):
        return jnp.where(row < 31, pltpu.roll(v, 31, 0), 0.0)

    def shift_down(v):
        return jnp.where(row > 0, pltpu.roll(v, 1, 0), 0.0)

    def window_tiles(win, base, carried, put):
        blocks = win.shape[0] // 32
        for t in range(blocks):
            piece = win[t * 32:t * 32 + 32, 0:128]
            if carried is not None:
                piece = piece + carried
            put(base + t, piece)
            carried = win[t * 32:t * 32 + 32, 128:256]
        return carried

    total_two = jnp.zeros((32, 256), F32)
    g_pairs = []
    carried = [None, None, None]
    done = 0
    for half in range(2):
        if half == 0:
            finish(p_pairs[0])
            finish(p_pairs[1])
        upto = (9, 17)[half]
        prepare_pool(halo_p.at[0], 0, done, upto)
        prepare_pool(halo_p.at[1], 2, done, upto)
        done = upto
        pre = pre_two[pl.ds(half * 256, 256), :] + bias_two
        pre = pre + dot(lhs_two((0, 2), half * 8, 8), jnp.concatenate([t2[0:768, :], t2[1536:2304, :]], axis=0))
        slp = slope_of(pre, sigmoid(pre))
        for b in range(8):
            block = half * 8 + b
            rows = pl.ds(block * 32, 32)
            delta = (cot_ref[0, 0, :, block * 256:block * 256 + 256].astype(F32) * slp[b * 32:b * 32 + 32]).astype(BF16)
            wide = delta.astype(F32)
            d2[1, rows, :] = delta
            d2[0, rows, :] = shift_up(wide).astype(BF16)
            d2[2, rows, :] = shift_down(wide).astype(BF16)
            total_two = total_two + wide
        rows = pl.ds(half * 256, 256)
        lhs = jnp.concatenate([d2[0, rows, :], d2[1, rows, :], d2[2, rows, :]], axis=1)
        for k in (0, 2):
            rhs = jnp.concatenate([t2[pl.ds((k * 3 + j) * 256, 256), :] for j in range(3)], axis=1)
            win = lax.dot_general(lhs, rhs, NT, preferred_element_type=F32)

            def put(t, piece, k=k):
                ref, t = (gs_a, t) if t < 8 else (gs_b, t - 8)
                ref[k // 2, :, t * 128:t * 128 + 128] = piece.astype(BF16)
            carried[k] = window_tiles(win, half * 8, carried[k], put)
            if half == 1:
                put(16, carried[k])
        put, got = ((gs_a, gr_a), (gs_b, gr_b))[half]
        g_pairs.append(exchange(put.at[0], put.at[1], got.at[1], got.at[0], 4 + half))

    two = jnp.sum(total_two, axis=0, keepdims=True)
    acc2[216 // 7, pl.ds((216 % 7) * 8, 8), :] = jnp.broadcast_to(two[:, 0:128] + two[:, 128:256], (8, 128))
    for unit in range(217, 224):
        acc2[unit // 7, pl.ds((unit % 7) * 8, 8), :] = jnp.zeros((8, 128), F32)
    for k in range(3):
        for j in range(3):
            lhs = jnp.concatenate([ps[k, j, :, b * 128:b * 128 + 256] for b in range(16)], axis=0)
            g = lax.dot_general(lhs, d2[1], TN, preferred_element_type=F32)
            s = g[0:192, 0:128] + g[64:256, 128:256]
            for part in range(24):
                unit = (k * 3 + j) * 24 + part
                acc2[unit // 7, pl.ds((unit % 7) * 8, 8), :] = s[part * 8:part * 8 + 8]

    def swap_start(a, acc, r0):
        cp = pltpu.make_async_remote_copy(
            src_ref=acc.at[pl.ds((1 - core) * 16, 16)], dst_ref=r0, send_sem=c_send.at[a, 0], recv_sem=c_recv.at[a, 0],
            device_id=partner, device_id_type=MESH)
        cp.start()
        return cp

    def plane_start(a, swap, acc, r0, half, r1):
        swap.wait()

        def add_half(i, carry):
            half[i] = (acc[core * 16 + i] + r0[i]).astype(half.dtype)
            return carry
        lax.fori_loop(0, 16, add_half, 0)
        sends = []
        for r in range(1, 16):
            da, db, q = chip_at(r)
            cp = pltpu.make_async_remote_copy(
                src_ref=half.at[q], dst_ref=r1.at[r - 1], send_sem=a_send.at[a, r - 1], recv_sem=a_recv.at[a, r - 1],
                device_id=(da, db), device_id_type=MESH)
            cp.start()
            sends.append(cp)
        return sends

    def column_start(a, sends, half, r1, r2):
        piece = half[chip + (core * 16 if a == 0 else 0)].astype(F32)
        for r in range(len(sends)):
            sends[r].wait()
            piece = piece + r1[r].astype(F32)
        r2[z] = piece.astype(r2.dtype)
        sends = []
        for r in range(1, 8):
            cp = pltpu.make_async_remote_copy(
                src_ref=r2.at[z], dst_ref=r2.at[z], send_sem=z_send.at[a, r - 1], recv_sem=z_recv.at[a, r - 1],
                device_id=z_at(r), device_id_type=MESH)
            cp.start()
            sends.append(cp)
        return sends

    def gather_start(a, sends, r2, final):
        for cp in sends:
            cp.wait()
        piece = r2[0].astype(F32)
        for i in range(1, 8):
            piece = piece + r2[i].astype(F32)
        mine = core * 16 + chip
        final[mine] = piece.astype(final.dtype)
        sends = []
        for r in range(1, 16):
            da, db, q = chip_at(r)
            cp = pltpu.make_async_remote_copy(
                src_ref=final.at[mine], dst_ref=final.at[mine], send_sem=g_send.at[a, r - 1], recv_sem=g_recv.at[a, r - 1],
                device_id=(da, db), device_id_type=MESH)
            cp.start()
            sends.append(cp)
        return sends

    def back_start(a, sends, final):
        for cp in sends:
            cp.wait()
        cp = pltpu.make_async_remote_copy(
            src_ref=final.at[pl.ds(core * 16, 16)], dst_ref=final.at[pl.ds(core * 16, 16)],
            send_sem=c_send.at[a, 1], recv_sem=c_recv.at[a, 1], device_id=partner, device_id_type=MESH)
        cp.start()
        return cp

    def scatter_start():
        def convert(i, carry):
            half1[i] = acc1[i].astype(half1.dtype)
            return carry
        lax.fori_loop(0, 32, convert, 0)
        sends = []
        for r in range(31):
            da, db, q = chip_at(r + 1) if r < 15 else other_at(r - 15)
            owner = (core if r < 15 else 1 - core) * 16 + q
            cp = pltpu.make_async_remote_copy(
                src_ref=half1.at[owner], dst_ref=r11.at[r], send_sem=b_send.at[0, r], recv_sem=b_recv.at[0, r],
                device_id=(da, db), device_id_type=MESH)
            cp.start()
            sends.append(cp)
        return sends

    def spread_start(sends):
        for cp in sends:
            cp.wait()
        piece = r21[0].astype(F32)
        for i in range(1, 8):
            piece = piece + r21[i].astype(F32)
        mine = core * 16 + chip
        fin1[mine] = piece.astype(fin1.dtype)
        sends = []
        for r in range(31):
            da, db, q = chip_at(r + 1) if r < 15 else other_at(r - 15)
            cp = pltpu.make_async_remote_copy(
                src_ref=fin1.at[mine], dst_ref=fin1.at[mine], send_sem=b_send.at[1, r], recv_sem=b_recv.at[1, r],
                device_id=(da, db), device_id_type=MESH)
            cp.start()
            sends.append(cp)
        return sends

    run2 = swap_start(1, acc2, r02)

    lhs = jnp.concatenate([d2[0], d2[1], d2[2]], axis=1)
    rhs = jnp.concatenate([t2[pl.ds((3 + j) * 256, 256), :] for j in range(3)], axis=1)

    def put_own(t, piece):
        gown[:, t * 128:t * 128 + 128] = piece
    put_own(16, window_tiles(lax.dot_general(lhs, rhs, NT, preferred_element_type=F32), 0, None, put_own))

    def pooled_tile(t, got, base):
        at = pl.ds(pl.multiple_of(t * 128, 128), 128)
        there = pl.ds(pl.multiple_of((t - base) * 128, 128), 128)
        v = gown[:, at] + got[0, :, there].astype(F32) + got[1, :, there].astype(F32)
        return pltpu.roll(v, 64, 1)

    def delta_one(got, base, b, carry):
        total, before = carry
        after = pooled_tile(b + 1, got, base)
        g = jnp.where(lane_p < 64, before, after)
        g = jnp.concatenate([g, g], axis=1)
        rows = pl.ds(pl.multiple_of(b * 32, 32), 32)
        for d in range(2):
            for p in range(2):
                delta = (g * slope[d * 2 + p, rows, :]).astype(BF16)
                wide = delta.astype(F32)
                d1[d, E0 if p == 0 else O0, rows, :] = delta
                if p == 0:
                    d1[d, EP, rows, :] = shift_up(wide).astype(BF16)
                else:
                    d1[d, OM, rows, :] = shift_down(wide).astype(BF16)
                total = total + wide
        return total, after

    finish(g_pairs[0])
    carry = lax.fori_loop(
        0, 7, functools.partial(delta_one, gr_a, 0), (jnp.zeros((32, 256), F32), pooled_tile(0, gr_a, 0)))
    finish(g_pairs[1])
    run2 = plane_start(1, run2, acc2, r02, half2, r12)
    total_one, _ = lax.fori_loop(7, 16, functools.partial(delta_one, gr_b, 8), carry)

    def window_one(terms, q):
        lhs = jnp.concatenate([d1[d, BWD[q][j]] for d, k in terms for j in range(3)], axis=1)
        rhs = jnp.concatenate([t1[pl.ds((k * 3 + j) * 256, 256), :] for d, k in terms for j in range(3)], axis=1)
        return lax.dot_general(lhs, rhs, NT, preferred_element_type=F32)

    x_pairs = []
    for q in range(2):
        for side, terms in ((0, ((0, 0),)), (1, ((1, 2),))):
            def put(t, piece, side=side, q=q):
                xsend[side, q, :, t * 128:t * 128 + 128] = piece.astype(BF16)
            put(16, window_tiles(window_one(terms, q), 0, None, put))
        x_pairs.append(exchange(xsend.at[0, q], xsend.at[1, q], xrecv.at[1, q], xrecv.at[0, q], 6 + q))
    for d in range(2):
        for p in range(2):
            for c in range(4):
                v = d1[d, p, pl.ds(c * 128, 128), :]
                d1t[:, pl.ds((d * 2 + p) * 512 + c * 128, 128)] = jnp.transpose(v)

    total = jnp.sum(total_one, axis=0, keepdims=True)
    total = total[:, 0:128] + total[:, 128:256]
    total = total + pltpu.roll(total, 64, 1)
    total_col = jnp.sum(
        jnp.where(lane == lax.broadcasted_iota(jnp.int32, (64, 128), 0), total, 0.0), axis=1, keepdims=True)

    def tap_one(tap):
        k, j = tap // 3, tap % 3
        rhs = jnp.concatenate([
            xv[d + k, FWD[p][j], :, b * 128:b * 128 + 256]
            for d in range(2) for p in range(2) for b in range(16)], axis=0)
        g = dot(d1t[...], rhs)
        s = g[0:64, 0:128] + pltpu.roll(g[128:192, 0:128], 128 - 32, 1)
        s = s + pltpu.roll(g[64:128, 0:256], 256 - 64, 1)[:, 0:128]
        return s + pltpu.roll(g[192:256, 0:256], 256 - 96, 1)[:, 0:128]

    last = tap_one(8)
    for tap in range(8):
        s = tap_one(tap)
        extra = pltpu.roll(last, 96 - 32 * tap, 1) if tap < 3 else total_col
        s = jnp.where(lane < 96, s, extra)
        for part in range(8):
            unit = tap * 8 + part
            acc1[unit // 2, pl.ds((unit % 2) * 8, 8), :] = s[part * 8:part * 8 + 8]
    run1 = scatter_start()

    run2 = column_start(1, run2, half2, r12, r22)

    def own_planes(e, terms):
        for q in range(2):
            def put(t, piece, q=q):
                xown[e, q, :, t * 128:t * 128 + 128] = piece
            put(16, window_tiles(window_one(terms, q), 0, None, put))
    own_planes(0, ((0, 1), (1, 0)))
    own_planes(1, ((0, 2), (1, 1)))
    run1 = column_start(0, run1, half1, r11, r21)
    run2 = gather_start(1, run2, r22, fin2)
    run1 = spread_start(run1)
    run2 = back_start(1, run2, fin2)

    for q in range(2):
        finish(x_pairs[q])
        for e in range(2):
            def tile(t):
                at = pl.ds(t * 128, 128)
                v = xown[e, q, :, at]
                v = v + xrecv[e, q, :, at].astype(F32)
                return pltpu.roll(v, 96, 1)
            before = tile(0)
            for t in range(16):
                after = tile(t + 1)
                outf[e, t, pl.ds(q, 32, stride=2), :] = jnp.where(lane_p < 96, before, after)
                before = after
    for e in range(2):
        for t in range(16):
            gx_buf[0, e, :, t * 128:t * 128 + 128] = outf[e, t].astype(BF16)

    run2.wait()
    for cp in run1:
        cp.wait()


def unpack(scale_one, scale_two, gx_in, final1, final2, gx_ref, gw1_ref, gb1_ref, gw2_ref, gb2_ref):
    gx_ref[...] = gx_in[...]

    def unit_two(unit):
        return final2[unit // 7, pl.ds((unit % 7) * 8, 8), :].astype(F32)

    for tap in range(9):
        for i in range(3):
            for part in range(8):
                gw2_ref[tap // 3, tap % 3, i, pl.ds(part * 8, 8), :] = unit_two(tap * 24 + i * 8 + part) * scale_two
    gb2_ref[...] = unit_two(216)[0:1] * scale_two
    for tap in range(8):
        turned = jnp.transpose(final1[pl.ds(tap * 4, 4)].reshape(64, 128).astype(F32)) * scale_one
        for i in range(3):
            gw1_ref[tap // 3, tap % 3, i] = turned[i * 32:i * 32 + 32]
        if tap < 3:
            gw1_ref[2, 2, tap] = turned[96:128]
        if tap == 3:
            gb1_ref[...] = turned[96:97]


def local(act_in, weight_one, bias_one, weight_two, bias_two, cotangent):
    scale_one = 16.0 / math.sqrt(16 * 32 * 64 * 64)
    scale_two = 1.0 / math.sqrt(16 * 16 * 32 * 32)
    vmem = pl.BlockSpec(memory_space=pltpu.VMEM)
    anywhere = pl.BlockSpec(memory_space=pltpu.HBM)
    scratch = [
        pltpu.VMEM((2, 64, 1152), BF16),
        pltpu.VMEM((2, 64, 896), BF16),
        pltpu.VMEM((3, 3, 3, 32, 64), BF16),
        pltpu.VMEM((1, 64), F32),
        pltpu.VMEM((3, 3, 3, 64, 128), BF16),
        pltpu.VMEM((1, 128), F32),
        pltpu.VMEM((1, 1, 32, 4096), BF16),
        pltpu.VMEM((2304, 256), BF16),
        pltpu.VMEM((2304, 256), BF16),
        pltpu.VMEM((17, 80, 128), F32),
        pltpu.VMEM((4, 4, 32, 2176), BF16),
        pltpu.VMEM((2, 64, 1152), BF16),
        pltpu.VMEM((2, 64, 896), BF16),
        pltpu.VMEM((4, 512, 256), F32),
        pltpu.VMEM((48, 2176), F32),
        pltpu.VMEM((2, 32, 1024), BF16),
        pltpu.VMEM((2, 2, 32, 1024), BF16),
        pltpu.VMEM((3, 3, 32, 2176), BF16),
        pltpu.VMEM((512, 256), F32),
        pltpu.VMEM((3, 512, 256), BF16),
        pltpu.VMEM((2, 32, 1024), BF16),
        pltpu.VMEM((2, 32, 1152), BF16),
        pltpu.VMEM((2, 32, 1024), BF16),
        pltpu.VMEM((2, 32, 1152), BF16),
        pltpu.VMEM((32, 2176), F32),
        pltpu.VMEM((2, 4, 512, 256), BF16),
        pltpu.VMEM((256, 2048), BF16),
        pltpu.VMEM((2, 2, 32, 2176), BF16),
        pltpu.VMEM((2, 2, 32, 2176), BF16),
        pltpu.VMEM((2, 2, 32, 2176), F32),
        pltpu.VMEM((2, 16, 64, 128), F32),
        pltpu.VMEM((32, ROWS1, 128), F32),
        pltpu.VMEM((32, ROWS1, 128), LINK1),
        pltpu.VMEM((31, ROWS1, 128), LINK1),
        pltpu.VMEM((8, ROWS1, 128), LINK1),
        pltpu.VMEM((32, ROWS2, 128), F32),
        pltpu.VMEM((16, ROWS2, 128), F32),
        pltpu.VMEM((16, ROWS2, 128), LINK2),
        pltpu.VMEM((15, ROWS2, 128), LINK2),
        pltpu.VMEM((8, ROWS2, 128), LINK2),
        pltpu.SemaphoreType.DMA((7,)),
        pltpu.SemaphoreType.DMA((8, 2)),
        pltpu.SemaphoreType.DMA((8, 2)),
        pltpu.SemaphoreType.DMA((2, 15)),
        pltpu.SemaphoreType.DMA((2, 15)),
        pltpu.SemaphoreType.DMA((2, 7)),
        pltpu.SemaphoreType.DMA((2, 7)),
        pltpu.SemaphoreType.DMA((2, 15)),
        pltpu.SemaphoreType.DMA((2, 15)),
        pltpu.SemaphoreType.DMA((2, 2)),
        pltpu.SemaphoreType.DMA((2, 2)),
        pltpu.SemaphoreType.DMA((2, 31)),
        pltpu.SemaphoreType.DMA((2, 31)),
    ]
    gx, final1, final2 = pl.pallas_call(
        kernel,
        out_shape=(
            jax.ShapeDtypeStruct((1, 2, 64, 2048), BF16),
            jax.ShapeDtypeStruct((32, ROWS1, 128), LINK1),
            jax.ShapeDtypeStruct((32, ROWS2, 128), LINK2),
        ),
        in_specs=[anywhere] * 6,
        out_specs=(vmem,) * 3,
        scratch_shapes=scratch,
        compiler_params=pltpu.CompilerParams(
            collective_id=0, has_side_effects=True, vmem_limit_bytes=32 * 1024 * 1024),
    )(*(pltpu.with_memory_space_constraint(v, pltpu.HBM) for v in (
        act_in, weight_one, bias_one.reshape(1, 64), weight_two, bias_two.reshape(1, 128), cotangent)))
    gx, gw1, gb1, gw2, gb2 = pl.pallas_call(
        functools.partial(unpack, scale_one, scale_two),
        out_shape=(
            jax.ShapeDtypeStruct((1, 2, 64, 2048), BF16),
            jax.ShapeDtypeStruct((3, 3, 3, 32, 64), F32),
            jax.ShapeDtypeStruct((1, 64), F32),
            jax.ShapeDtypeStruct((3, 3, 3, 64, 128), F32),
            jax.ShapeDtypeStruct((1, 128), F32),
        ),
        in_specs=[vmem] * 3,
        out_specs=(vmem,) * 5,
        compiler_params=pltpu.CompilerParams(vmem_limit_bytes=16 * 1024 * 1024),
    )(gx, final1, final2)
    return gx, gw1, gb1.reshape(64), gw2, gb2.reshape(128)


def solution(mesh):
    placed = (P("dp", "space", None, None), P(), P(), P(), P(), P("dp", "space", None, None))
    return jax.shard_map(
        local,
        mesh=mesh,
        in_specs=placed,
        out_specs=(P("dp", "space", None, None), P(), P(), P(), P()),
        check_vma=False,
    )
```

```python
import functools
import math

import jax
import jax.numpy as jnp
from jax import lax
from jax.experimental import pallas as pl
from jax.experimental.pallas import tpu as pltpu
from jax.sharding import PartitionSpec as P

F32 = jnp.float32
BF16 = jnp.bfloat16
LINK1 = jnp.bfloat16
LINK2 = jnp.bfloat16
MESH = pl.DeviceIdType.MESH

E0, O0, EP, OM = 0, 1, 2, 3
FWD = ((OM, E0, O0), (E0, O0, EP))
BWD = ((O0, E0, OM), (EP, O0, E0))

NT = (((1,), (1,)), ((), ()))
TN = (((0,), (0,)), ((), ()))

X_CUT = (0, 9, 16)
ROWS2 = 56
ROWS1 = 16


def dot(a, b):
    return jnp.dot(a, b, preferred_element_type=F32)


def slope_of(value, sig):
    return sig * (1.0 + value * (1.0 - sig))


def sigmoid(value):
    return 0.5 * jnp.tanh(0.5 * value) + 0.5


def kernel(
    x_hbm, w1_hbm, b1_hbm, w2_hbm, b2_hbm, cot_hbm,
    gx_buf, fin1, fin2,
    x_a, x_b, w1_ref, b1_ref, w2_ref, b2_ref, cot_ref,
    t1, t2, xf, xv, halo_a, halo_b, slope, pf, pool, halo_p, ps, pre_two, d2, gs_a, gs_b, gr_a, gr_b, gown,
    d1, d1t, xsend, xrecv, xown, outf,
    half1, r11, r21,
    acc2, r02, half2, r12, r22,
    l_sem, s_send, s_recv, a_send, a_recv, z_send, z_recv, g_send, g_recv, c_send, c_recv, b_send, b_recv,
):
    dp = lax.axis_index("dp")
    space = lax.axis_index("space")
    nxt = lax.rem(space + 1, 16)
    prv = lax.rem(space + 15, 16)
    core = lax.rem(dp, 2)
    x_pos = lax.rem(dp // 2, 2) * 2 + space // 8
    chip = (dp // 4) * 4 + x_pos
    z = lax.rem(space, 8)
    partner = (dp + 1 - 2 * core, space)

    def chip_at(r):
        q = lax.rem(chip + r, 16)
        qx = lax.rem(q, 4)
        return (q // 4) * 4 + (qx // 2) * 2 + core, lax.rem(qx, 2) * 8 + z, q

    def other_at(r):
        da, db, q = chip_at(r)
        return da + 1 - 2 * core, db, q

    def z_at(r):
        return dp, (space // 8) * 8 + lax.rem(z + r, 8)

    barrier = pltpu.get_barrier_semaphore()

    def greet(device):
        pl.semaphore_signal(barrier, inc=1, device_id=device, device_id_type=MESH)

    loads = []
    for i, (src, dst) in enumerate((
        (x_hbm.at[0, :, :, pl.ds(0, 1152)], x_a), (x_hbm.at[0, :, :, pl.ds(1152, 896)], x_b),
        (w1_hbm, w1_ref), (w2_hbm, w2_ref), (b1_hbm, b1_ref), (b2_hbm, b2_ref), (cot_hbm, cot_ref),
    )):
        cp = pltpu.make_async_copy(src, dst, l_sem.at[i])
        cp.start()
        loads.append(cp)

    greet((dp, nxt))
    greet((dp, prv))
    for r in range(1, 8):
        greet(z_at(r))
    for r in range(1, 16):
        greet(chip_at(r)[:2])
    for r in range(16):
        greet(other_at(r)[:2])

    not_last = space < 15
    not_first = space > 0

    def exchange(down, up, from_next, from_prev, stage):
        one = pltpu.make_async_remote_copy(
            src_ref=down, dst_ref=from_next, send_sem=s_send.at[stage, 0], recv_sem=s_recv.at[stage, 0],
            device_id=(dp, prv), device_id_type=MESH)
        two = pltpu.make_async_remote_copy(
            src_ref=up, dst_ref=from_prev, send_sem=s_send.at[stage, 1], recv_sem=s_recv.at[stage, 1],
            device_id=(dp, nxt), device_id_type=MESH)

        @pl.when(not_first)
        def _():
            one.start()

        @pl.when(not_last)
        def _():
            two.start()
        return one, two

    def finish(pair):
        one, two = pair

        @pl.when(not_first)
        def _():
            one.wait_send()
            two.wait_recv()

        @pl.when(not_last)
        def _():
            two.wait_send()
            one.wait_recv()

    loads[0].wait()
    loads[1].wait()
    pl.semaphore_wait(barrier, 40)
    x_pairs = [
        exchange(x_a.at[0], x_a.at[1], halo_a.at[1], halo_a.at[0], 0),
        exchange(x_b.at[0], x_b.at[1], halo_b.at[1], halo_b.at[0], 1),
    ]

    @pl.when(jnp.logical_not(not_first))
    def _():
        halo_a[0] = jnp.zeros(halo_a.shape[1:], BF16)
        halo_b[0] = jnp.zeros(halo_b.shape[1:], BF16)
        halo_p[0] = jnp.zeros(halo_p.shape[1:], BF16)
        gr_a[0] = jnp.zeros(gr_a.shape[1:], BF16)
        gr_b[0] = jnp.zeros(gr_b.shape[1:], BF16)
        xrecv[0] = jnp.zeros(xrecv.shape[1:], BF16)

    @pl.when(jnp.logical_not(not_last))
    def _():
        halo_a[1] = jnp.zeros(halo_a.shape[1:], BF16)
        halo_b[1] = jnp.zeros(halo_b.shape[1:], BF16)
        halo_p[1] = jnp.zeros(halo_p.shape[1:], BF16)
        gr_a[1] = jnp.zeros(gr_a.shape[1:], BF16)
        gr_b[1] = jnp.zeros(gr_b.shape[1:], BF16)
        xrecv[1] = jnp.zeros(xrecv.shape[1:], BF16)

    lane = lax.broadcasted_iota(jnp.int32, (64, 128), 1)

    def prepare(src, side, plane, first, last):
        def turned(t):
            if t < 0 or t > 15:
                return jnp.zeros((64, 128), F32)
            c = 0 if t < X_CUT[1] else 1
            v = src[c][side, :, (t - X_CUT[c]) * 128:(t - X_CUT[c]) * 128 + 128].astype(F32)
            return pltpu.roll(v, 32, 1)
        before = turned(first - 1)
        for t in range(first, last):
            here = turned(t)
            xf[t, 8:72, :] = jnp.where(lane < 32, before, here)
            before = here
            at = pl.ds(t * 128, 128)
            xv[plane, E0, :, at] = xf[t, pl.ds(8, 32, stride=2), :].astype(BF16)
            xv[plane, O0, :, at] = xf[t, pl.ds(9, 32, stride=2), :].astype(BF16)
            xv[plane, EP, :, at] = xf[t, pl.ds(10, 32, stride=2), :].astype(BF16)
            xv[plane, OM, :, at] = xf[t, pl.ds(7, 32, stride=2), :].astype(BF16)

    xf[:, 0:8, :] = jnp.zeros((17, 8, 128), F32)
    xf[:, 72:80, :] = jnp.zeros((17, 8, 128), F32)
    pf[0:8, :] = jnp.zeros((8, 2176), F32)
    pf[40:48, :] = jnp.zeros((8, 2176), F32)

    loads[2].wait()
    for k in range(3):
        for j in range(3):
            w = w1_ref[k, j].reshape(96, 64).astype(F32)
            for t in range(2):
                cols = []
                for v in (t, t + 2):
                    parts = [w]
                    if v:
                        parts = [jnp.zeros((32 * v, 64), F32)] + parts
                    parts = parts + [jnp.zeros((160 - 32 * v, 64), F32)]
                    cols.append(jnp.concatenate(parts, axis=0))
                t1[pl.ds((k * 3 + j) * 256, 256), pl.ds(t * 128, 128)] = jnp.concatenate(cols, axis=1).astype(BF16)

    prepare((x_a, x_b), 0, 1, 0, 17)
    prepare((x_a, x_b), 1, 2, 0, 17)

    for i in range(3, 7):
        loads[i].wait()
    for k in range(3):
        for j in range(3):
            w = w2_ref[k, j].reshape(192, 128)
            gap = jnp.zeros((64, 128), BF16)
            t2[pl.ds((k * 3 + j) * 256, 256), pl.ds(0, 128)] = jnp.concatenate([w, gap], axis=0)
            t2[pl.ds((k * 3 + j) * 256, 256), pl.ds(128, 128)] = jnp.concatenate([gap, w], axis=0)

    bias = jnp.concatenate([b1_ref[...], b1_ref[...]], axis=1)
    bias = jnp.concatenate([bias, bias], axis=1)

    def lhs_one(d, ks, first, blocks):
        return jnp.concatenate([
            jnp.concatenate([
                xv[d + k, FWD[p][j], :, pl.ds(pl.multiple_of((first + b) * 128, 128), 256)]
                for p in range(2) for b in range(blocks)], axis=0)
            for k in ks for j in range(3)], axis=1)

    def own_one(g, carry):
        for d in range(2):
            part = dot(lhs_one(d, (1 - d, 2 - d), g * 8, 8), t1[pl.ds((1 - d) * 768, 1536), :])
            for p in range(2):
                slope[d * 2 + p, pl.ds(pl.multiple_of(g * 256, 256), 256), :] = part[p * 256:p * 256 + 256]
        return carry
    lax.fori_loop(0, 2, own_one, 0)

    p_pairs = []
    for g in range(2):
        finish(x_pairs[g])
        prepare((halo_a, halo_b), 0, 0, (0, 9)[g], (9, 17)[g])
        prepare((halo_a, halo_b), 1, 3, (0, 9)[g], (9, 17)[g])
        sums = [None] * 8
        rows = pl.ds(g * 256, 256)
        for d in range(2):
            part = dot(lhs_one(d, (2 * d,), g * 8, 8), t1[pl.ds(2 * d * 768, 768), :])
            for p in range(2):
                pre = part[p * 256:p * 256 + 256] + slope[d * 2 + p, rows, :] + bias
                sig = sigmoid(pre)
                act = pre * sig
                slope[d * 2 + p, rows, :] = slope_of(pre, sig) * 0.125
                for b in range(8):
                    piece = act[b * 32:b * 32 + 32, 0:128] + act[b * 32:b * 32 + 32, 128:256]
                    sums[b] = piece if sums[b] is None else sums[b] + piece
        for b in range(8):
            pool[g, :, b * 128:b * 128 + 128] = (sums[b] * 0.125).astype(BF16)
        p_pairs.append(exchange(pool.at[g], pool.at[g], halo_p.at[1, g], halo_p.at[0, g], 2 + g))

    lane_p = lax.broadcasted_iota(jnp.int32, (32, 128), 1)

    def prepare_pool(src, plane, first, last):
        def turned(t):
            if t < 0 or t > 15:
                return jnp.zeros((32, 128), F32)
            v = src[t // 8, :, t % 8 * 128:t % 8 * 128 + 128].astype(F32)
            return pltpu.roll(v, 64, 1)
        before = turned(first - 1)
        for t in range(first, last):
            here = turned(t)
            at = pl.ds(t * 128, 128)
            pf[8:40, at] = jnp.where(lane_p < 64, before, here)
            before = here
            for j in range(3):
                ps[plane, j, :, at] = pf[7 + j:39 + j, at].astype(BF16)

    def lhs_two(ks, first, blocks):
        return jnp.concatenate([
            jnp.concatenate([ps[k, j, :, pl.ds((first + b) * 128, 256)] for b in range(blocks)], axis=0)
            for k in ks for j in range(3)], axis=1)

    prepare_pool(pool, 1, 0, 17)
    pre_two[...] = dot(lhs_two((1,), 0, 16), t2[pl.ds(768, 768), :])

    row = lax.broadcasted_iota(jnp.int32, (32, 256), 0)
    bias_two = jnp.concatenate([b2_ref[...], b2_ref[...]], axis=1)

    def shift_up(v):
        return jnp.where(row < 31, pltpu.roll(v, 31, 0), 0.0)

    def shift_down(v):
        return jnp.where(row > 0, pltpu.roll(v, 1, 0), 0.0)

    def window_tiles(win, base, carried, put):
        blocks = win.shape[0] // 32
        for t in range(blocks):
            piece = win[t * 32:t * 32 + 32, 0:128]
            if carried is not None:
                piece = piece + carried
            put(base + t, piece)
            carried = win[t * 32:t * 32 + 32, 128:256]
        return carried

    total_two = jnp.zeros((32, 256), F32)
    g_pairs = []
    carried = [None, None, None]
    done = 0
    for half in range(2):
        if half == 0:
            finish(p_pairs[0])
            finish(p_pairs[1])
        upto = (9, 17)[half]
        prepare_pool(halo_p.at[0], 0, done, upto)
        prepare_pool(halo_p.at[1], 2, done, upto)
        done = upto
        pre = pre_two[pl.ds(half * 256, 256), :] + bias_two
        pre = pre + dot(lhs_two((0, 2), half * 8, 8), jnp.concatenate([t2[0:768, :], t2[1536:2304, :]], axis=0))
        slp = slope_of(pre, sigmoid(pre))
        for b in range(8):
            block = half * 8 + b
            rows = pl.ds(block * 32, 32)
            delta = (cot_ref[0, 0, :, block * 256:block * 256 + 256].astype(F32) * slp[b * 32:b * 32 + 32]).astype(BF16)
            wide = delta.astype(F32)
            d2[1, rows, :] = delta
            d2[0, rows, :] = shift_up(wide).astype(BF16)
            d2[2, rows, :] = shift_down(wide).astype(BF16)
            total_two = total_two + wide
        rows = pl.ds(half * 256, 256)
        lhs = jnp.concatenate([d2[0, rows, :], d2[1, rows, :], d2[2, rows, :]], axis=1)
        for k in (0, 2):
            rhs = jnp.concatenate([t2[pl.ds((k * 3 + j) * 256, 256), :] for j in range(3)], axis=1)
            win = lax.dot_general(lhs, rhs, NT, preferred_element_type=F32)

            def put(t, piece, k=k):
                ref, t = (gs_a, t) if t < 8 else (gs_b, t - 8)
                ref[k // 2, :, t * 128:t * 128 + 128] = piece.astype(BF16)
            carried[k] = window_tiles(win, half * 8, carried[k], put)
            if half == 1:
                put(16, carried[k])
        put, got = ((gs_a, gr_a), (gs_b, gr_b))[half]
        g_pairs.append(exchange(put.at[0], put.at[1], got.at[1], got.at[0], 4 + half))

    two = jnp.sum(total_two, axis=0, keepdims=True)
    acc2[216 // 7, pl.ds((216 % 7) * 8, 8), :] = jnp.broadcast_to(two[:, 0:128] + two[:, 128:256], (8, 128))
    for unit in range(217, 224):
        acc2[unit // 7, pl.ds((unit % 7) * 8, 8), :] = jnp.zeros((8, 128), F32)
    for k in range(3):
        for j in range(3):
            lhs = jnp.concatenate([ps[k, j, :, b * 128:b * 128 + 256] for b in range(16)], axis=0)
            g = lax.dot_general(lhs, d2[1], TN, preferred_element_type=F32)
            s = g[0:192, 0:128] + g[64:256, 128:256]
            for part in range(24):
                unit = (k * 3 + j) * 24 + part
                acc2[unit // 7, pl.ds((unit % 7) * 8, 8), :] = s[part * 8:part * 8 + 8]

    def all_of(src, dst, send, recv):
        return pltpu.make_async_remote_copy(
            src_ref=src, dst_ref=dst, send_sem=send, recv_sem=recv, device_id=partner, device_id_type=MESH)

    def swap_start(a, acc, r0):
        cp = pltpu.make_async_remote_copy(
            src_ref=acc.at[pl.ds((1 - core) * 16, 16)], dst_ref=r0, send_sem=c_send.at[0], recv_sem=c_recv.at[0],
            device_id=partner, device_id_type=MESH)
        cp.start()
        return cp

    def plane_start(a, swap, acc, r0, half, r1):
        swap.wait()

        def add_half(i, carry):
            half[i] = (acc[core * 16 + i] + r0[i]).astype(half.dtype)
            return carry
        lax.fori_loop(0, 16, add_half, 0)
        for r in range(1, 16):
            da, db, q = chip_at(r)
            pltpu.make_async_remote_copy(
                src_ref=half.at[q], dst_ref=r1.at[r - 1], send_sem=a_send.at[0], recv_sem=a_recv.at[0],
                device_id=(da, db), device_id_type=MESH).start()
        return all_of(half.at[0:15], r1, a_send.at[0], a_recv.at[0])

    def column_start(a, sends, half, r1, r2):
        piece = half[chip + (core * 16 if a == 0 else 0)].astype(F32)
        sends.wait()
        for r in range(r1.shape[0]):
            piece = piece + r1[r].astype(F32)
        r2[z] = piece.astype(r2.dtype)
        for r in range(1, 8):
            pltpu.make_async_remote_copy(
                src_ref=r2.at[z], dst_ref=r2.at[z], send_sem=z_send.at[a], recv_sem=z_recv.at[a],
                device_id=z_at(r), device_id_type=MESH).start()
        return all_of(r2.at[0:7], r2.at[0:7], z_send.at[a], z_recv.at[a])

    def gather_start(a, sends, r2, final):
        sends.wait()
        piece = r2[0].astype(F32)
        for i in range(1, 8):
            piece = piece + r2[i].astype(F32)
        mine = core * 16 + chip
        final[mine] = piece.astype(final.dtype)
        for r in range(1, 16):
            da, db, q = chip_at(r)
            pltpu.make_async_remote_copy(
                src_ref=final.at[mine], dst_ref=final.at[mine], send_sem=g_send.at[0], recv_sem=g_recv.at[0],
                device_id=(da, db), device_id_type=MESH).start()
        return all_of(final.at[0:15], final.at[0:15], g_send.at[0], g_recv.at[0])

    def back_start(a, sends, final):
        sends.wait()
        cp = pltpu.make_async_remote_copy(
            src_ref=final.at[pl.ds(core * 16, 16)], dst_ref=final.at[pl.ds(core * 16, 16)],
            send_sem=c_send.at[1], recv_sem=c_recv.at[1], device_id=partner, device_id_type=MESH)
        cp.start()
        return cp

    def scatter_start():
        for r in range(31):
            da, db, q = chip_at(r + 1) if r < 15 else other_at(r - 15)
            owner = (core if r < 15 else 1 - core) * 16 + q
            pltpu.make_async_remote_copy(
                src_ref=half1.at[owner], dst_ref=r11.at[r], send_sem=b_send.at[0], recv_sem=b_recv.at[0],
                device_id=(da, db), device_id_type=MESH).start()
        return all_of(half1.at[0:31], r11, b_send.at[0], b_recv.at[0])

    def spread_start(sends):
        sends.wait()
        piece = r21[0].astype(F32)
        for i in range(1, 8):
            piece = piece + r21[i].astype(F32)
        mine = core * 16 + chip
        fin1[mine] = piece.astype(fin1.dtype)
        for r in range(31):
            da, db, q = chip_at(r + 1) if r < 15 else other_at(r - 15)
            pltpu.make_async_remote_copy(
                src_ref=fin1.at[mine], dst_ref=fin1.at[mine], send_sem=b_send.at[1], recv_sem=b_recv.at[1],
                device_id=(da, db), device_id_type=MESH).start()
        return all_of(fin1.at[0:31], fin1.at[0:31], b_send.at[1], b_recv.at[1])

    run2 = swap_start(1, acc2, r02)

    lhs = jnp.concatenate([d2[0], d2[1], d2[2]], axis=1)
    rhs = jnp.concatenate([t2[pl.ds((3 + j) * 256, 256), :] for j in range(3)], axis=1)

    def put_own(t, piece):
        gown[:, t * 128:t * 128 + 128] = piece
    put_own(16, window_tiles(lax.dot_general(lhs, rhs, NT, preferred_element_type=F32), 0, None, put_own))

    def pooled_tile(t, got, base):
        at = pl.ds(pl.multiple_of(t * 128, 128), 128)
        there = pl.ds(pl.multiple_of((t - base) * 128, 128), 128)
        v = gown[:, at] + got[0, :, there].astype(F32) + got[1, :, there].astype(F32)
        return pltpu.roll(v, 64, 1)

    def delta_one(got, base, b, carry):
        total, before = carry
        after = pooled_tile(b + 1, got, base)
        g = jnp.where(lane_p < 64, before, after)
        g = jnp.concatenate([g, g], axis=1)
        rows = pl.ds(pl.multiple_of(b * 32, 32), 32)
        for d in range(2):
            for p in range(2):
                delta = (g * slope[d * 2 + p, rows, :]).astype(BF16)
                wide = delta.astype(F32)
                d1[d, E0 if p == 0 else O0, rows, :] = delta
                if p == 0:
                    d1[d, EP, rows, :] = shift_up(wide).astype(BF16)
                else:
                    d1[d, OM, rows, :] = shift_down(wide).astype(BF16)
                total = total + wide
        return total, after

    finish(g_pairs[0])
    carry = lax.fori_loop(
        0, 7, functools.partial(delta_one, gr_a, 0), (jnp.zeros((32, 256), F32), pooled_tile(0, gr_a, 0)), unroll=True)
    finish(g_pairs[1])
    run2 = plane_start(1, run2, acc2, r02, half2, r12)
    total_one, _ = lax.fori_loop(7, 16, functools.partial(delta_one, gr_b, 8), carry, unroll=True)

    def window_one(terms, q):
        lhs = jnp.concatenate([d1[d, BWD[q][j]] for d, k in terms for j in range(3)], axis=1)
        rhs = jnp.concatenate([t1[pl.ds((k * 3 + j) * 256, 256), :] for d, k in terms for j in range(3)], axis=1)
        return lax.dot_general(lhs, rhs, NT, preferred_element_type=F32)

    x_pairs = []
    for q in range(2):
        for side, terms in ((0, ((0, 0),)), (1, ((1, 2),))):
            def put(t, piece, side=side, q=q):
                xsend[side, q, :, t * 128:t * 128 + 128] = piece.astype(BF16)
            put(16, window_tiles(window_one(terms, q), 0, None, put))
        x_pairs.append(exchange(xsend.at[0, q], xsend.at[1, q], xrecv.at[1, q], xrecv.at[0, q], 6 + q))
    for d in range(2):
        for p in range(2):
            for c in range(4):
                v = d1[d, p, pl.ds(c * 128, 128), :]
                d1t[:, pl.ds((d * 2 + p) * 512 + c * 128, 128)] = jnp.transpose(v)

    total = jnp.sum(total_one, axis=0, keepdims=True)
    total = total[:, 0:128] + total[:, 128:256]
    total = total + pltpu.roll(total, 64, 1)
    total_col = jnp.sum(
        jnp.where(lane == lax.broadcasted_iota(jnp.int32, (64, 128), 0), total, 0.0), axis=1, keepdims=True)

    def tap_one(tap):
        k, j = tap // 3, tap % 3
        rhs = jnp.concatenate([
            xv[d + k, FWD[p][j], :, b * 128:b * 128 + 256]
            for d in range(2) for p in range(2) for b in range(16)], axis=0)
        g = dot(d1t[...], rhs)
        s = g[0:64, 0:128] + pltpu.roll(g[128:192, 0:128], 128 - 32, 1)
        s = s + pltpu.roll(g[64:128, 0:256], 256 - 64, 1)[:, 0:128]
        return s + pltpu.roll(g[192:256, 0:256], 256 - 96, 1)[:, 0:128]

    last = tap_one(8)
    for tap in range(8):
        s = tap_one(tap)
        extra = pltpu.roll(last, 96 - 32 * tap, 1) if tap < 3 else total_col
        s = jnp.where(lane < 96, s, extra)
        for part in range(4):
            half1[tap * 4 + part] = s[part * 16:part * 16 + 16].astype(LINK1)
    run1 = scatter_start()

    run2 = column_start(1, run2, half2, r12, r22)

    def own_planes(e, terms):
        for q in range(2):
            def put(t, piece, q=q):
                xown[e, q, :, t * 128:t * 128 + 128] = piece
            put(16, window_tiles(window_one(terms, q), 0, None, put))
    own_planes(0, ((0, 1), (1, 0)))
    own_planes(1, ((0, 2), (1, 1)))
    run1 = column_start(0, run1, half1, r11, r21)
    run2 = gather_start(1, run2, r22, fin2)
    run1 = spread_start(run1)
    for q in range(2):
        finish(x_pairs[q])
        for e in range(2):
            def tile(t):
                at = pl.ds(t * 128, 128)
                v = xown[e, q, :, at]
                v = v + xrecv[e, q, :, at].astype(F32)
                return pltpu.roll(v, 96, 1)
            before = tile(0)
            for t in range(16):
                after = tile(t + 1)
                outf[e, t, pl.ds(q, 32, stride=2), :] = jnp.where(lane_p < 96, before, after)
                before = after
    for e in range(2):
        for t in range(16):
            gx_buf[0, e, :, t * 128:t * 128 + 128] = outf[e, t].astype(BF16)

    run2 = back_start(1, run2, fin2)

    run2.wait()
    run1.wait()


def unpack(scale_one, scale_two, gx_in, final1, final2, gx_ref, gw1_ref, gb1_ref, gw2_ref, gb2_ref):
    gx_ref[...] = gx_in[...]

    def unit_two(unit):
        return final2[unit // 7, pl.ds((unit % 7) * 8, 8), :].astype(F32)

    for tap in range(9):
        for i in range(3):
            for part in range(8):
                gw2_ref[tap // 3, tap % 3, i, pl.ds(part * 8, 8), :] = unit_two(tap * 24 + i * 8 + part) * scale_two
    gb2_ref[...] = unit_two(216)[0:1] * scale_two
    for tap in range(8):
        turned = jnp.transpose(final1[pl.ds(tap * 4, 4)].reshape(64, 128).astype(F32)) * scale_one
        for i in range(3):
            gw1_ref[tap // 3, tap % 3, i] = turned[i * 32:i * 32 + 32]
        if tap < 3:
            gw1_ref[2, 2, tap] = turned[96:128]
        if tap == 3:
            gb1_ref[...] = turned[96:97]


def local(act_in, weight_one, bias_one, weight_two, bias_two, cotangent):
    scale_one = 16.0 / math.sqrt(16 * 32 * 64 * 64)
    scale_two = 1.0 / math.sqrt(16 * 16 * 32 * 32)
    vmem = pl.BlockSpec(memory_space=pltpu.VMEM)
    anywhere = pl.BlockSpec(memory_space=pltpu.HBM)
    scratch = [
        pltpu.VMEM((2, 64, 1152), BF16),
        pltpu.VMEM((2, 64, 896), BF16),
        pltpu.VMEM((3, 3, 3, 32, 64), BF16),
        pltpu.VMEM((1, 64), F32),
        pltpu.VMEM((3, 3, 3, 64, 128), BF16),
        pltpu.VMEM((1, 128), F32),
        pltpu.VMEM((1, 1, 32, 4096), BF16),
        pltpu.VMEM((2304, 256), BF16),
        pltpu.VMEM((2304, 256), BF16),
        pltpu.VMEM((17, 80, 128), F32),
        pltpu.VMEM((4, 4, 32, 2176), BF16),
        pltpu.VMEM((2, 64, 1152), BF16),
        pltpu.VMEM((2, 64, 896), BF16),
        pltpu.VMEM((4, 512, 256), F32),
        pltpu.VMEM((48, 2176), F32),
        pltpu.VMEM((2, 32, 1024), BF16),
        pltpu.VMEM((2, 2, 32, 1024), BF16),
        pltpu.VMEM((3, 3, 32, 2176), BF16),
        pltpu.VMEM((512, 256), F32),
        pltpu.VMEM((3, 512, 256), BF16),
        pltpu.VMEM((2, 32, 1024), BF16),
        pltpu.VMEM((2, 32, 1152), BF16),
        pltpu.VMEM((2, 32, 1024), BF16),
        pltpu.VMEM((2, 32, 1152), BF16),
        pltpu.VMEM((32, 2176), F32),
        pltpu.VMEM((2, 4, 512, 256), BF16),
        pltpu.VMEM((256, 2048), BF16),
        pltpu.VMEM((2, 2, 32, 2176), BF16),
        pltpu.VMEM((2, 2, 32, 2176), BF16),
        pltpu.VMEM((2, 2, 32, 2176), F32),
        pltpu.VMEM((2, 16, 64, 128), F32),
        pltpu.VMEM((32, ROWS1, 128), LINK1),
        pltpu.VMEM((31, ROWS1, 128), LINK1),
        pltpu.VMEM((8, ROWS1, 128), LINK1),
        pltpu.VMEM((32, ROWS2, 128), F32),
        pltpu.VMEM((16, ROWS2, 128), F32),
        pltpu.VMEM((16, ROWS2, 128), LINK2),
        pltpu.VMEM((15, ROWS2, 128), LINK2),
        pltpu.VMEM((8, ROWS2, 128), LINK2),
        pltpu.SemaphoreType.DMA((7,)),
        pltpu.SemaphoreType.DMA((8, 2)),
        pltpu.SemaphoreType.DMA((8, 2)),
        pltpu.SemaphoreType.DMA((1,)),
        pltpu.SemaphoreType.DMA((1,)),
        pltpu.SemaphoreType.DMA((2,)),
        pltpu.SemaphoreType.DMA((2,)),
        pltpu.SemaphoreType.DMA((1,)),
        pltpu.SemaphoreType.DMA((1,)),
        pltpu.SemaphoreType.DMA((2,)),
        pltpu.SemaphoreType.DMA((2,)),
        pltpu.SemaphoreType.DMA((2,)),
        pltpu.SemaphoreType.DMA((2,)),
    ]
    gx, final1, final2 = pl.pallas_call(
        kernel,
        out_shape=(
            jax.ShapeDtypeStruct((1, 2, 64, 2048), BF16),
            jax.ShapeDtypeStruct((32, ROWS1, 128), LINK1),
            jax.ShapeDtypeStruct((32, ROWS2, 128), LINK2),
        ),
        in_specs=[anywhere] * 6,
        out_specs=(vmem,) * 3,
        scratch_shapes=scratch,
        compiler_params=pltpu.CompilerParams(
            collective_id=0, has_side_effects=True, vmem_limit_bytes=32 * 1024 * 1024),
    )(*(pltpu.with_memory_space_constraint(v, pltpu.HBM) for v in (
        act_in, weight_one, bias_one.reshape(1, 64), weight_two, bias_two.reshape(1, 128), cotangent)))
    gx, gw1, gb1, gw2, gb2 = pl.pallas_call(
        functools.partial(unpack, scale_one, scale_two),
        out_shape=(
            jax.ShapeDtypeStruct((1, 2, 64, 2048), BF16),
            jax.ShapeDtypeStruct((3, 3, 3, 32, 64), F32),
            jax.ShapeDtypeStruct((1, 64), F32),
            jax.ShapeDtypeStruct((3, 3, 3, 64, 128), F32),
            jax.ShapeDtypeStruct((1, 128), F32),
        ),
        in_specs=[vmem] * 3,
        out_specs=(vmem,) * 5,
        compiler_params=pltpu.CompilerParams(vmem_limit_bytes=16 * 1024 * 1024),
    )(gx, final1, final2)
    return gx, gw1, gb1.reshape(64), gw2, gb2.reshape(128)


def solution(mesh):
    placed = (P("dp", "space", None, None), P(), P(), P(), P(), P("dp", "space", None, None))
    return jax.shard_map(
        local,
        mesh=mesh,
        in_specs=placed,
        out_specs=(P("dp", "space", None, None), P(), P(), P(), P()),
        check_vma=False,
    )
```

```python
import functools
import math

import jax
import jax.numpy as jnp
from jax import lax
from jax.experimental import pallas as pl
from jax.experimental.pallas import tpu as pltpu
from jax.sharding import PartitionSpec as P

F32 = jnp.float32
BF16 = jnp.bfloat16
LINK1 = jnp.bfloat16
LINK2 = jnp.bfloat16
MESH = pl.DeviceIdType.MESH

E0, O0, EP, OM = 0, 1, 2, 3
FWD = ((OM, E0, O0), (E0, O0, EP))
BWD = ((O0, E0, OM), (EP, O0, E0))

NT = (((1,), (1,)), ((), ()))
TN = (((0,), (0,)), ((), ()))

X_CUT = (0, 9, 16)
ROWS2 = 56
ROWS1 = 16


def dot(a, b):
    return jnp.dot(a, b, preferred_element_type=F32)


def slope_of(value, sig):
    return sig * (1.0 + value * (1.0 - sig))


def sigmoid(value):
    return 0.5 * jnp.tanh(0.5 * value) + 0.5


def kernel(
    x_hbm, w1_hbm, b1_hbm, w2_hbm, b2_hbm, cot_hbm,
    gx_buf, fin1, fin2,
    x_a, x_b, w1_ref, b1_ref, w2_ref, b2_ref, cot_ref,
    t1, t2, xf, xv, halo_a, halo_b, slope, pf, pool, halo_p, ps, pre_two, d2, gs_a, gs_b, gr_a, gr_b, gown,
    d1, d1t, g_part, xsend, xrecv, xown, outf,
    half1, r11, r21,
    acc2, r02, half2, r12, r22,
    l_sem, s_send, s_recv, a_send, a_recv, z_send, z_recv, g_send, g_recv, c_send, c_recv, b_send, b_recv,
):
    dp = lax.axis_index("dp")
    space = lax.axis_index("space")
    nxt = lax.rem(space + 1, 16)
    prv = lax.rem(space + 15, 16)
    core = lax.rem(dp, 2)
    x_pos = lax.rem(dp // 2, 2) * 2 + space // 8
    chip = (dp // 4) * 4 + x_pos
    z = lax.rem(space, 8)
    partner = (dp + 1 - 2 * core, space)

    def chip_at(r):
        q = lax.rem(chip + r, 16)
        qx = lax.rem(q, 4)
        return (q // 4) * 4 + (qx // 2) * 2 + core, lax.rem(qx, 2) * 8 + z, q

    def other_at(r):
        da, db, q = chip_at(r)
        return da + 1 - 2 * core, db, q

    def z_at(r):
        return dp, (space // 8) * 8 + lax.rem(z + r, 8)

    barrier = pltpu.get_barrier_semaphore()

    def greet(device):
        pl.semaphore_signal(barrier, inc=1, device_id=device, device_id_type=MESH)

    loads = []
    for i, (src, dst) in enumerate((
        (x_hbm.at[0, :, :, pl.ds(0, 1152)], x_a), (x_hbm.at[0, :, :, pl.ds(1152, 896)], x_b),
        (w1_hbm, w1_ref), (w2_hbm, w2_ref), (b1_hbm, b1_ref), (b2_hbm, b2_ref), (cot_hbm, cot_ref),
    )):
        cp = pltpu.make_async_copy(src, dst, l_sem.at[i])
        cp.start()
        loads.append(cp)

    greet((dp, nxt))
    greet((dp, prv))
    for r in range(1, 8):
        greet(z_at(r))
    for r in range(1, 16):
        greet(chip_at(r)[:2])
    for r in range(16):
        greet(other_at(r)[:2])

    not_last = space < 15
    not_first = space > 0

    def exchange(down, up, from_next, from_prev, stage):
        one = pltpu.make_async_remote_copy(
            src_ref=down, dst_ref=from_next, send_sem=s_send.at[stage, 0], recv_sem=s_recv.at[stage, 0],
            device_id=(dp, prv), device_id_type=MESH)
        two = pltpu.make_async_remote_copy(
            src_ref=up, dst_ref=from_prev, send_sem=s_send.at[stage, 1], recv_sem=s_recv.at[stage, 1],
            device_id=(dp, nxt), device_id_type=MESH)

        @pl.when(not_first)
        def _():
            one.start()

        @pl.when(not_last)
        def _():
            two.start()
        return one, two

    def finish(pair):
        one, two = pair

        @pl.when(not_first)
        def _():
            one.wait_send()
            two.wait_recv()

        @pl.when(not_last)
        def _():
            two.wait_send()
            one.wait_recv()

    loads[0].wait()
    loads[1].wait()
    pl.semaphore_wait(barrier, 40)
    x_pairs = [
        exchange(x_a.at[0], x_a.at[1], halo_a.at[1], halo_a.at[0], 0),
        exchange(x_b.at[0], x_b.at[1], halo_b.at[1], halo_b.at[0], 1),
    ]

    @pl.when(jnp.logical_not(not_first))
    def _():
        halo_a[0] = jnp.zeros(halo_a.shape[1:], BF16)
        halo_b[0] = jnp.zeros(halo_b.shape[1:], BF16)
        halo_p[0] = jnp.zeros(halo_p.shape[1:], BF16)
        gr_a[0] = jnp.zeros(gr_a.shape[1:], BF16)
        gr_b[0] = jnp.zeros(gr_b.shape[1:], BF16)
        xrecv[0] = jnp.zeros(xrecv.shape[1:], BF16)

    @pl.when(jnp.logical_not(not_last))
    def _():
        halo_a[1] = jnp.zeros(halo_a.shape[1:], BF16)
        halo_b[1] = jnp.zeros(halo_b.shape[1:], BF16)
        halo_p[1] = jnp.zeros(halo_p.shape[1:], BF16)
        gr_a[1] = jnp.zeros(gr_a.shape[1:], BF16)
        gr_b[1] = jnp.zeros(gr_b.shape[1:], BF16)
        xrecv[1] = jnp.zeros(xrecv.shape[1:], BF16)

    lane = lax.broadcasted_iota(jnp.int32, (64, 128), 1)

    def prepare(src, side, plane, first, last):
        def turned(t):
            if t < 0 or t > 15:
                return jnp.zeros((64, 128), F32)
            c = 0 if t < X_CUT[1] else 1
            v = src[c][side, :, (t - X_CUT[c]) * 128:(t - X_CUT[c]) * 128 + 128].astype(F32)
            return pltpu.roll(v, 32, 1)
        before = turned(first - 1)
        for t in range(first, last):
            here = turned(t)
            xf[t, 8:72, :] = jnp.where(lane < 32, before, here)
            before = here
            at = pl.ds(t * 128, 128)
            xv[plane, E0, :, at] = xf[t, pl.ds(8, 32, stride=2), :].astype(BF16)
            xv[plane, O0, :, at] = xf[t, pl.ds(9, 32, stride=2), :].astype(BF16)
            xv[plane, EP, :, at] = xf[t, pl.ds(10, 32, stride=2), :].astype(BF16)
            xv[plane, OM, :, at] = xf[t, pl.ds(7, 32, stride=2), :].astype(BF16)

    xf[:, 0:8, :] = jnp.zeros((17, 8, 128), F32)
    xf[:, 72:80, :] = jnp.zeros((17, 8, 128), F32)
    pf[0:8, :] = jnp.zeros((8, 2176), F32)
    pf[40:48, :] = jnp.zeros((8, 2176), F32)

    loads[2].wait()
    for k in range(3):
        for j in range(3):
            w = w1_ref[k, j].reshape(96, 64).astype(F32)
            for t in range(2):
                cols = []
                for v in (t, t + 2):
                    parts = [w]
                    if v:
                        parts = [jnp.zeros((32 * v, 64), F32)] + parts
                    parts = parts + [jnp.zeros((160 - 32 * v, 64), F32)]
                    cols.append(jnp.concatenate(parts, axis=0))
                t1[pl.ds((k * 3 + j) * 256, 256), pl.ds(t * 128, 128)] = jnp.concatenate(cols, axis=1).astype(BF16)

    prepare((x_a, x_b), 0, 1, 0, 17)
    prepare((x_a, x_b), 1, 2, 0, 17)

    for i in range(3, 7):
        loads[i].wait()
    for k in range(3):
        for j in range(3):
            w = w2_ref[k, j].reshape(192, 128)
            gap = jnp.zeros((64, 128), BF16)
            t2[pl.ds((k * 3 + j) * 256, 256), pl.ds(0, 128)] = jnp.concatenate([w, gap], axis=0)
            t2[pl.ds((k * 3 + j) * 256, 256), pl.ds(128, 128)] = jnp.concatenate([gap, w], axis=0)

    bias = jnp.concatenate([b1_ref[...], b1_ref[...]], axis=1)
    bias = jnp.concatenate([bias, bias], axis=1)

    def lhs_one(d, ks, first, blocks):
        return jnp.concatenate([
            jnp.concatenate([
                xv[d + k, FWD[p][j], :, pl.ds(pl.multiple_of((first + b) * 128, 128), 256)]
                for p in range(2) for b in range(blocks)], axis=0)
            for k in ks for j in range(3)], axis=1)

    def own_one(g, carry):
        for d in range(2):
            part = dot(lhs_one(d, (1 - d, 2 - d), g * 8, 8), t1[pl.ds((1 - d) * 768, 1536), :])
            for p in range(2):
                slope[d * 2 + p, pl.ds(pl.multiple_of(g * 256, 256), 256), :] = part[p * 256:p * 256 + 256]
        return carry
    lax.fori_loop(0, 2, own_one, 0)

    p_pairs = []
    for g in range(2):
        finish(x_pairs[g])
        prepare((halo_a, halo_b), 0, 0, (0, 9)[g], (9, 17)[g])
        prepare((halo_a, halo_b), 1, 3, (0, 9)[g], (9, 17)[g])
        sums = [None] * 8
        rows = pl.ds(g * 256, 256)
        for d in range(2):
            part = dot(lhs_one(d, (2 * d,), g * 8, 8), t1[pl.ds(2 * d * 768, 768), :])
            for p in range(2):
                pre = part[p * 256:p * 256 + 256] + slope[d * 2 + p, rows, :] + bias
                sig = sigmoid(pre)
                act = pre * sig
                slope[d * 2 + p, rows, :] = slope_of(pre, sig) * 0.125
                for b in range(8):
                    piece = act[b * 32:b * 32 + 32, 0:128] + act[b * 32:b * 32 + 32, 128:256]
                    sums[b] = piece if sums[b] is None else sums[b] + piece
        for b in range(8):
            pool[g, :, b * 128:b * 128 + 128] = (sums[b] * 0.125).astype(BF16)
        p_pairs.append(exchange(pool.at[g], pool.at[g], halo_p.at[1, g], halo_p.at[0, g], 2 + g))

    lane_p = lax.broadcasted_iota(jnp.int32, (32, 128), 1)

    def prepare_pool(src, plane, first, last):
        def turned(t):
            if t < 0 or t > 15:
                return jnp.zeros((32, 128), F32)
            v = src[t // 8, :, t % 8 * 128:t % 8 * 128 + 128].astype(F32)
            return pltpu.roll(v, 64, 1)
        before = turned(first - 1)
        for t in range(first, last):
            here = turned(t)
            at = pl.ds(t * 128, 128)
            pf[8:40, at] = jnp.where(lane_p < 64, before, here)
            before = here
            for j in range(3):
                ps[plane, j, :, at] = pf[7 + j:39 + j, at].astype(BF16)

    def lhs_two(ks, first, blocks):
        return jnp.concatenate([
            jnp.concatenate([ps[k, j, :, pl.ds((first + b) * 128, 256)] for b in range(blocks)], axis=0)
            for k in ks for j in range(3)], axis=1)

    prepare_pool(pool, 1, 0, 17)
    pre_two[...] = dot(lhs_two((1,), 0, 16), t2[pl.ds(768, 768), :])

    row = lax.broadcasted_iota(jnp.int32, (32, 256), 0)
    bias_two = jnp.concatenate([b2_ref[...], b2_ref[...]], axis=1)

    def shift_up(v):
        return jnp.where(row < 31, pltpu.roll(v, 31, 0), 0.0)

    def shift_down(v):
        return jnp.where(row > 0, pltpu.roll(v, 1, 0), 0.0)

    def window_tiles(win, base, carried, put):
        blocks = win.shape[0] // 32
        for t in range(blocks):
            piece = win[t * 32:t * 32 + 32, 0:128]
            if carried is not None:
                piece = piece + carried
            put(base + t, piece)
            carried = win[t * 32:t * 32 + 32, 128:256]
        return carried

    total_two = jnp.zeros((32, 256), F32)
    g_pairs = []
    carried = [None, None, None]
    done = 0
    for half in range(2):
        finish(p_pairs[half])
        upto = (8, 17)[half]
        first, count = ((0, 7), (7, 9))[half]
        prepare_pool(halo_p.at[0], 0, done, upto)
        prepare_pool(halo_p.at[1], 2, done, upto)
        done = upto
        pre = pre_two[pl.ds(first * 32, count * 32), :] + bias_two
        pre = pre + dot(lhs_two((0, 2), first, count), jnp.concatenate([t2[0:768, :], t2[1536:2304, :]], axis=0))
        slp = slope_of(pre, sigmoid(pre))
        for b in range(count):
            block = first + b
            rows = pl.ds(block * 32, 32)
            delta = (cot_ref[0, 0, :, block * 256:block * 256 + 256].astype(F32) * slp[b * 32:b * 32 + 32]).astype(BF16)
            wide = delta.astype(F32)
            d2[1, rows, :] = delta
            d2[0, rows, :] = shift_up(wide).astype(BF16)
            d2[2, rows, :] = shift_down(wide).astype(BF16)
            total_two = total_two + wide
        rows = pl.ds(first * 32, count * 32)
        lhs = jnp.concatenate([d2[0, rows, :], d2[1, rows, :], d2[2, rows, :]], axis=1)
        for k in (0, 2):
            rhs = jnp.concatenate([t2[pl.ds((k * 3 + j) * 256, 256), :] for j in range(3)], axis=1)
            win = lax.dot_general(lhs, rhs, NT, preferred_element_type=F32)

            def put(t, piece, k=k):
                ref, t = (gs_a, t) if t < 7 else (gs_b, t - 7)
                ref[k // 2, :, t * 128:t * 128 + 128] = piece.astype(BF16)
            carried[k] = window_tiles(win, first, carried[k], put)
            if half == 1:
                put(16, carried[k])
        put, got = ((gs_a, gr_a), (gs_b, gr_b))[half]
        g_pairs.append(exchange(put.at[0], put.at[1], got.at[1], got.at[0], 4 + half))

    two = jnp.sum(total_two, axis=0, keepdims=True)
    acc2[216 // 7, pl.ds((216 % 7) * 8, 8), :] = jnp.broadcast_to(two[:, 0:128] + two[:, 128:256], (8, 128))
    for unit in range(217, 224):
        acc2[unit // 7, pl.ds((unit % 7) * 8, 8), :] = jnp.zeros((8, 128), F32)
    for k in range(3):
        for j in range(3):
            lhs = jnp.concatenate([ps[k, j, :, b * 128:b * 128 + 256] for b in range(16)], axis=0)
            g = lax.dot_general(lhs, d2[1], TN, preferred_element_type=F32)
            s = g[0:192, 0:128] + g[64:256, 128:256]
            for part in range(24):
                unit = (k * 3 + j) * 24 + part
                acc2[unit // 7, pl.ds((unit % 7) * 8, 8), :] = s[part * 8:part * 8 + 8]

    def all_of(src, dst, send, recv):
        return pltpu.make_async_remote_copy(
            src_ref=src, dst_ref=dst, send_sem=send, recv_sem=recv, device_id=partner, device_id_type=MESH)

    def swap_start(a, acc, r0):
        cp = pltpu.make_async_remote_copy(
            src_ref=acc.at[pl.ds((1 - core) * 16, 16)], dst_ref=r0, send_sem=c_send.at[0], recv_sem=c_recv.at[0],
            device_id=partner, device_id_type=MESH)
        cp.start()
        return cp

    def plane_start(a, swap, acc, r0, half, r1):
        swap.wait()

        def add_half(i, carry):
            half[i] = (acc[core * 16 + i] + r0[i]).astype(half.dtype)
            return carry
        lax.fori_loop(0, 16, add_half, 0)
        for r in range(1, 16):
            da, db, q = chip_at(r)
            pltpu.make_async_remote_copy(
                src_ref=half.at[q], dst_ref=r1.at[r - 1], send_sem=a_send.at[0], recv_sem=a_recv.at[0],
                device_id=(da, db), device_id_type=MESH).start()
        return all_of(half.at[0:15], r1, a_send.at[0], a_recv.at[0])

    def column_start(a, sends, half, r1, r2):
        piece = half[chip + (core * 16 if a == 0 else 0)].astype(F32)
        sends.wait()
        for r in range(r1.shape[0]):
            piece = piece + r1[r].astype(F32)
        r2[z] = piece.astype(r2.dtype)
        for r in range(1, 8):
            pltpu.make_async_remote_copy(
                src_ref=r2.at[z], dst_ref=r2.at[z], send_sem=z_send.at[a], recv_sem=z_recv.at[a],
                device_id=z_at(r), device_id_type=MESH).start()
        return all_of(r2.at[0:7], r2.at[0:7], z_send.at[a], z_recv.at[a])

    def gather_start(a, sends, r2, final):
        sends.wait()
        piece = r2[0].astype(F32)
        for i in range(1, 8):
            piece = piece + r2[i].astype(F32)
        mine = core * 16 + chip
        final[mine] = piece.astype(final.dtype)
        for r in range(1, 16):
            da, db, q = chip_at(r)
            pltpu.make_async_remote_copy(
                src_ref=final.at[mine], dst_ref=final.at[mine], send_sem=g_send.at[0], recv_sem=g_recv.at[0],
                device_id=(da, db), device_id_type=MESH).start()
        return all_of(final.at[0:15], final.at[0:15], g_send.at[0], g_recv.at[0])

    def back_start(a, sends, final):
        sends.wait()
        cp = pltpu.make_async_remote_copy(
            src_ref=final.at[pl.ds(core * 16, 16)], dst_ref=final.at[pl.ds(core * 16, 16)],
            send_sem=c_send.at[1], recv_sem=c_recv.at[1], device_id=partner, device_id_type=MESH)
        cp.start()
        return cp

    def scatter_start():
        for r in range(31):
            da, db, q = chip_at(r + 1) if r < 15 else other_at(r - 15)
            owner = (core if r < 15 else 1 - core) * 16 + q
            pltpu.make_async_remote_copy(
                src_ref=half1.at[owner], dst_ref=r11.at[r], send_sem=b_send.at[0], recv_sem=b_recv.at[0],
                device_id=(da, db), device_id_type=MESH).start()
        return all_of(half1.at[0:31], r11, b_send.at[0], b_recv.at[0])

    def spread_start(sends):
        sends.wait()
        piece = r21[0].astype(F32)
        for i in range(1, 8):
            piece = piece + r21[i].astype(F32)
        mine = core * 16 + chip
        fin1[mine] = piece.astype(fin1.dtype)
        for r in range(31):
            da, db, q = chip_at(r + 1) if r < 15 else other_at(r - 15)
            pltpu.make_async_remote_copy(
                src_ref=fin1.at[mine], dst_ref=fin1.at[mine], send_sem=b_send.at[1], recv_sem=b_recv.at[1],
                device_id=(da, db), device_id_type=MESH).start()
        return all_of(fin1.at[0:31], fin1.at[0:31], b_send.at[1], b_recv.at[1])

    run2 = swap_start(1, acc2, r02)

    lhs = jnp.concatenate([d2[0], d2[1], d2[2]], axis=1)
    rhs = jnp.concatenate([t2[pl.ds((3 + j) * 256, 256), :] for j in range(3)], axis=1)

    def put_own(t, piece):
        gown[:, t * 128:t * 128 + 128] = piece
    put_own(16, window_tiles(lax.dot_general(lhs, rhs, NT, preferred_element_type=F32), 0, None, put_own))

    def pooled_tile(t, got, base):
        at = pl.ds(pl.multiple_of(t * 128, 128), 128)
        there = pl.ds(pl.multiple_of((t - base) * 128, 128), 128)
        v = gown[:, at] + got[0, :, there].astype(F32) + got[1, :, there].astype(F32)
        return pltpu.roll(v, 64, 1)

    def delta_one(got, base, b, carry):
        total, before = carry
        after = pooled_tile(b + 1, got, base)
        g = jnp.where(lane_p < 64, before, after)
        g = jnp.concatenate([g, g], axis=1)
        rows = pl.ds(pl.multiple_of(b * 32, 32), 32)
        for d in range(2):
            for p in range(2):
                delta = (g * slope[d * 2 + p, rows, :]).astype(BF16)
                wide = delta.astype(F32)
                d1[d, E0 if p == 0 else O0, rows, :] = delta
                if p == 0:
                    d1[d, EP, rows, :] = shift_up(wide).astype(BF16)
                else:
                    d1[d, OM, rows, :] = shift_down(wide).astype(BF16)
                total = total + wide
        return total, after

    finish(g_pairs[0])
    carry = lax.fori_loop(
        0, 6, functools.partial(delta_one, gr_a, 0), (jnp.zeros((32, 256), F32), pooled_tile(0, gr_a, 0)), unroll=True)
    def window_part(terms, q, first, count):
        rows = pl.ds(first * 32, count * 32)
        lhs = jnp.concatenate([d1[d, BWD[q][j], rows, :] for d, k in terms for j in range(3)], axis=1)
        rhs = jnp.concatenate([t1[pl.ds((k * 3 + j) * 256, 256), :] for d, k in terms for j in range(3)], axis=1)
        return lax.dot_general(lhs, rhs, NT, preferred_element_type=F32)

    def turn(c):
        for d in range(2):
            for p in range(2):
                v = d1[d, p, pl.ds(c * 128, 128), :]
                d1t[:, pl.ds((d * 2 + p) * 512 + c * 128, 128)] = jnp.transpose(v)

    def tap_dot(tap, first, last):
        k, j = tap // 3, tap % 3
        lhs = jnp.concatenate([
            d1t[:, (d * 2 + p) * 512 + first * 32:(d * 2 + p) * 512 + last * 32]
            for d in range(2) for p in range(2)], axis=1)
        rhs = jnp.concatenate([
            xv[d + k, FWD[p][j], :, b * 128:b * 128 + 256]
            for d in range(2) for p in range(2) for b in range(first, last)], axis=0)
        return dot(lhs, rhs)

    def put_side(side, q):
        def put(t, piece):
            xsend[side, q, :, t * 128:t * 128 + 128] = piece.astype(BF16)
        return put

    turn(0)
    for tap in range(9):
        g_part[tap] = tap_dot(tap, 0, 4)
    sides = (((0, 0),), ((1, 2),))
    over = {}
    for q in range(2):
        for side in range(2):
            win = window_part(sides[side], q, 0, 6)
            over[side, q] = window_tiles(win, 0, None, put_side(side, q))

    finish(g_pairs[1])
    run2 = plane_start(1, run2, acc2, r02, half2, r12)
    total_one, _ = lax.fori_loop(6, 16, functools.partial(delta_one, gr_b, 7), carry, unroll=True)

    def window_one(terms, q):
        lhs = jnp.concatenate([d1[d, BWD[q][j]] for d, k in terms for j in range(3)], axis=1)
        rhs = jnp.concatenate([t1[pl.ds((k * 3 + j) * 256, 256), :] for d, k in terms for j in range(3)], axis=1)
        return lax.dot_general(lhs, rhs, NT, preferred_element_type=F32)

    x_pairs = []
    for q in range(2):
        for side in range(2):
            put = put_side(side, q)
            put(16, window_tiles(window_part(sides[side], q, 6, 10), 6, over[side, q], put))
        x_pairs.append(exchange(xsend.at[0, q], xsend.at[1, q], xrecv.at[1, q], xrecv.at[0, q], 6 + q))
    for c in range(1, 4):
        turn(c)

    total = jnp.sum(total_one, axis=0, keepdims=True)
    total = total[:, 0:128] + total[:, 128:256]
    total = total + pltpu.roll(total, 64, 1)
    total_col = jnp.sum(
        jnp.where(lane == lax.broadcasted_iota(jnp.int32, (64, 128), 0), total, 0.0), axis=1, keepdims=True)

    def tap_one(tap):
        g = g_part[tap] + tap_dot(tap, 4, 16)
        s = g[0:64, 0:128] + pltpu.roll(g[128:192, 0:128], 128 - 32, 1)
        s = s + pltpu.roll(g[64:128, 0:256], 256 - 64, 1)[:, 0:128]
        return s + pltpu.roll(g[192:256, 0:256], 256 - 96, 1)[:, 0:128]

    last = tap_one(8)
    for tap in range(8):
        s = tap_one(tap)
        extra = pltpu.roll(last, 96 - 32 * tap, 1) if tap < 3 else total_col
        s = jnp.where(lane < 96, s, extra)
        for part in range(4):
            half1[tap * 4 + part] = s[part * 16:part * 16 + 16].astype(LINK1)
    run1 = scatter_start()

    run2 = column_start(1, run2, half2, r12, r22)

    def own_planes(e, terms):
        for q in range(2):
            def put(t, piece, q=q):
                xown[e, q, :, t * 128:t * 128 + 128] = piece
            put(16, window_tiles(window_one(terms, q), 0, None, put))
    own_planes(0, ((0, 1), (1, 0)))
    own_planes(1, ((0, 2), (1, 1)))
    run1 = column_start(0, run1, half1, r11, r21)
    run2 = gather_start(1, run2, r22, fin2)
    run1 = spread_start(run1)
    for q in range(2):
        finish(x_pairs[q])
        for e in range(2):
            def tile(t):
                at = pl.ds(t * 128, 128)
                v = xown[e, q, :, at]
                v = v + xrecv[e, q, :, at].astype(F32)
                return pltpu.roll(v, 96, 1)
            before = tile(0)
            for t in range(16):
                after = tile(t + 1)
                outf[e, t, pl.ds(q, 32, stride=2), :] = jnp.where(lane_p < 96, before, after)
                before = after
    for e in range(2):
        for t in range(16):
            gx_buf[0, e, :, t * 128:t * 128 + 128] = outf[e, t].astype(BF16)

    run2 = back_start(1, run2, fin2)

    run2.wait()
    run1.wait()


def unpack(scale_one, scale_two, gx_in, final1, final2, gx_ref, gw1_ref, gb1_ref, gw2_ref, gb2_ref):
    gx_ref[...] = gx_in[...]

    def unit_two(unit):
        return final2[unit // 7, pl.ds((unit % 7) * 8, 8), :].astype(F32)

    for tap in range(9):
        for i in range(3):
            for part in range(8):
                gw2_ref[tap // 3, tap % 3, i, pl.ds(part * 8, 8), :] = unit_two(tap * 24 + i * 8 + part) * scale_two
    gb2_ref[...] = unit_two(216)[0:1] * scale_two
    for tap in range(8):
        turned = jnp.transpose(final1[pl.ds(tap * 4, 4)].reshape(64, 128).astype(F32)) * scale_one
        for i in range(3):
            gw1_ref[tap // 3, tap % 3, i] = turned[i * 32:i * 32 + 32]
        if tap < 3:
            gw1_ref[2, 2, tap] = turned[96:128]
        if tap == 3:
            gb1_ref[...] = turned[96:97]


def local(act_in, weight_one, bias_one, weight_two, bias_two, cotangent):
    scale_one = 16.0 / math.sqrt(16 * 32 * 64 * 64)
    scale_two = 1.0 / math.sqrt(16 * 16 * 32 * 32)
    vmem = pl.BlockSpec(memory_space=pltpu.VMEM)
    anywhere = pl.BlockSpec(memory_space=pltpu.HBM)
    scratch = [
        pltpu.VMEM((2, 64, 1152), BF16),
        pltpu.VMEM((2, 64, 896), BF16),
        pltpu.VMEM((3, 3, 3, 32, 64), BF16),
        pltpu.VMEM((1, 64), F32),
        pltpu.VMEM((3, 3, 3, 64, 128), BF16),
        pltpu.VMEM((1, 128), F32),
        pltpu.VMEM((1, 1, 32, 4096), BF16),
        pltpu.VMEM((2304, 256), BF16),
        pltpu.VMEM((2304, 256), BF16),
        pltpu.VMEM((17, 80, 128), F32),
        pltpu.VMEM((4, 4, 32, 2176), BF16),
        pltpu.VMEM((2, 64, 1152), BF16),
        pltpu.VMEM((2, 64, 896), BF16),
        pltpu.VMEM((4, 512, 256), F32),
        pltpu.VMEM((48, 2176), F32),
        pltpu.VMEM((2, 32, 1024), BF16),
        pltpu.VMEM((2, 2, 32, 1024), BF16),
        pltpu.VMEM((3, 3, 32, 2176), BF16),
        pltpu.VMEM((512, 256), F32),
        pltpu.VMEM((3, 512, 256), BF16),
        pltpu.VMEM((2, 32, 896), BF16),
        pltpu.VMEM((2, 32, 1280), BF16),
        pltpu.VMEM((2, 32, 896), BF16),
        pltpu.VMEM((2, 32, 1280), BF16),
        pltpu.VMEM((32, 2176), F32),
        pltpu.VMEM((2, 4, 512, 256), BF16),
        pltpu.VMEM((256, 2048), BF16),
        pltpu.VMEM((9, 256, 256), F32),
        pltpu.VMEM((2, 2, 32, 2176), BF16),
        pltpu.VMEM((2, 2, 32, 2176), BF16),
        pltpu.VMEM((2, 2, 32, 2176), F32),
        pltpu.VMEM((2, 16, 64, 128), F32),
        pltpu.VMEM((32, ROWS1, 128), LINK1),
        pltpu.VMEM((31, ROWS1, 128), LINK1),
        pltpu.VMEM((8, ROWS1, 128), LINK1),
        pltpu.VMEM((32, ROWS2, 128), F32),
        pltpu.VMEM((16, ROWS2, 128), F32),
        pltpu.VMEM((16, ROWS2, 128), LINK2),
        pltpu.VMEM((15, ROWS2, 128), LINK2),
        pltpu.VMEM((8, ROWS2, 128), LINK2),
        pltpu.SemaphoreType.DMA((7,)),
        pltpu.SemaphoreType.DMA((8, 2)),
        pltpu.SemaphoreType.DMA((8, 2)),
        pltpu.SemaphoreType.DMA((1,)),
        pltpu.SemaphoreType.DMA((1,)),
        pltpu.SemaphoreType.DMA((2,)),
        pltpu.SemaphoreType.DMA((2,)),
        pltpu.SemaphoreType.DMA((1,)),
        pltpu.SemaphoreType.DMA((1,)),
        pltpu.SemaphoreType.DMA((2,)),
        pltpu.SemaphoreType.DMA((2,)),
        pltpu.SemaphoreType.DMA((2,)),
        pltpu.SemaphoreType.DMA((2,)),
    ]
    gx, final1, final2 = pl.pallas_call(
        kernel,
        out_shape=(
            jax.ShapeDtypeStruct((1, 2, 64, 2048), BF16),
            jax.ShapeDtypeStruct((32, ROWS1, 128), LINK1),
            jax.ShapeDtypeStruct((32, ROWS2, 128), LINK2),
        ),
        in_specs=[anywhere] * 6,
        out_specs=(vmem,) * 3,
        scratch_shapes=scratch,
        compiler_params=pltpu.CompilerParams(
            collective_id=0, has_side_effects=True, vmem_limit_bytes=32 * 1024 * 1024),
    )(*(pltpu.with_memory_space_constraint(v, pltpu.HBM) for v in (
        act_in, weight_one, bias_one.reshape(1, 64), weight_two, bias_two.reshape(1, 128), cotangent)))
    gx, gw1, gb1, gw2, gb2 = pl.pallas_call(
        functools.partial(unpack, scale_one, scale_two),
        out_shape=(
            jax.ShapeDtypeStruct((1, 2, 64, 2048), BF16),
            jax.ShapeDtypeStruct((3, 3, 3, 32, 64), F32),
            jax.ShapeDtypeStruct((1, 64), F32),
            jax.ShapeDtypeStruct((3, 3, 3, 64, 128), F32),
            jax.ShapeDtypeStruct((1, 128), F32),
        ),
        in_specs=[vmem] * 3,
        out_specs=(vmem,) * 5,
        compiler_params=pltpu.CompilerParams(vmem_limit_bytes=16 * 1024 * 1024),
    )(gx, final1, final2)
    return gx, gw1, gb1.reshape(64), gw2, gb2.reshape(128)


def solution(mesh):
    placed = (P("dp", "space", None, None), P(), P(), P(), P(), P("dp", "space", None, None))
    return jax.shard_map(
        local,
        mesh=mesh,
        in_specs=placed,
        out_specs=(P("dp", "space", None, None), P(), P(), P(), P()),
        check_vma=False,
    )
```
